32 devices in a mesh: vx: 4 (over y, x), vy: 8 (over z, core).
Axes of the slice: x: 2, y: 2, z: 4, core: 2. Of those that a mesh axis runs over, the one named last changes fastest.
Arguments:
- tokens: bfloat16 [96, 1, 256, 1024], P(('vx', 'vy')), may hold values from -256 to 256
- var_embed: bfloat16 [91, 1024], replicated, may hold values from -2 to 2
- query: bfloat16 [1024], replicated, may hold values from -6 to 6
- key_weight: bfloat16 [1024, 1024], P('vy'), may hold values from -1 to 1
- value_weight: bfloat16 [1024, 1024], P('vy'), may hold values from -0.1875 to 0.1875
- out_weight: bfloat16 [1024, 1024], P('vy'), may hold values from -0.1875 to 0.1875
- var_slot: int32 [91], replicated, may hold values from 0 to 95, as said below
Outputs:
- aggregated: bfloat16 [1, 256, 1024], P(None, ('vx', 'vy'))
The draws below stay inside these ranges and needn't reach their ends.
Inputs may be any that keep to these rules, and one draw needn't show every extreme that they name: `var_slot`: distinct slot numbers; at least one device's slot holds a variable.
All inputs are finite; a program needn't handle non-finite values.
Results may differ from the reference program's by a relative error of at most 0.0096.
Values may be sent and summed in bfloat16 or wider, within the bound.
A program may use at most 64 MiB of HBM per device.

```python
import math
import jax
import jax.numpy as jnp
from jax import lax

D = 1024
HEADS = 16
VARS = 91
B = 1
PATCH_DEV = 8
PATCH = 256
SLOT_DEV = 3
SLOTS = 96


def shared_params(key):
    first, second, third = jax.random.split(jax.random.fold_in(key, 7), 3)
    key_matrix = jax.random.truncated_normal(first, -6.0, 6.0, (D, D), jnp.float32) * D ** (-0.5)
    query_vector = jax.random.truncated_normal(second, -4.0, 4.0, (D,), jnp.float32) * 1.5
    embeddings = jax.random.truncated_normal(third, -4.0, 4.0, (VARS, D), jnp.float32) * 0.5
    return (key_matrix, query_vector, embeddings)


def slot_table(key):
    first, second, third = jax.random.split(jax.random.fold_in(key, 19), 3)
    ranking = jax.random.permutation(first, SLOTS).astype(jnp.int32)
    full_device = jax.random.randint(second, (), 0, SLOTS // SLOT_DEV)
    slot_index = jnp.arange(SLOTS, dtype=jnp.int32)
    priority = jnp.where(slot_index // SLOT_DEV == full_device, slot_index % SLOT_DEV - SLOT_DEV, ranking)
    ordering = jnp.argsort(priority, stable=True)
    occupied = ordering[:VARS]
    return occupied[jax.random.permutation(third, VARS)].astype(jnp.int32)


def draw_var_slot(key, part):
    return slot_table(key)


def draw_key_weight(key, part):
    return shared_params(key)[0].astype(jnp.bfloat16)


def draw_query(key, part):
    return shared_params(key)[1].astype(jnp.bfloat16)


def draw_var_embed(key, part):
    return shared_params(key)[2].astype(jnp.bfloat16)


def draw_tokens(key, part):
    keys_all = jax.random.split(jax.random.fold_in(key, 31), 1)
    return jax.random.truncated_normal(keys_all[0], -6.0, 6.0, (SLOTS, B, PATCH, D), jnp.float32).astype(jnp.bfloat16)


def steps_of(stream_key, extent, cuts, low, largest):
    def one(dim, parts):
        heights = jax.random.uniform(jax.random.fold_in(jax.random.fold_in(stream_key, 6), dim), (parts,), jnp.float32, low / len(cuts), largest / len(cuts))
        return jnp.repeat(jnp.exp(heights), extent[dim] // parts).reshape((-1,) + (1,) * (len(extent) - dim - 1))

    factor_of = one(*cuts[0])
    for cut in cuts[1:]:
        factor_of = factor_of * one(*cut)
    return factor_of


def bell_draw(rng, dims, deviation, reach, cuts=(), kind=jnp.bfloat16):
    array = deviation * jax.random.normal(rng, dims, jnp.float32)
    if cuts:
        array = array * steps_of(rng, dims, cuts, -0.22, 0.18)
    return jnp.clip(array, -reach, reach).astype(kind)


def setup_inputs(seed: int = 0) -> dict:
    key_list = jax.random.split(jax.random.key(seed), 8)
    return {
        "tokens": draw_tokens(jax.random.fold_in(key_list[7], 71), 0),
        "var_embed": draw_var_embed(jax.random.fold_in(key_list[7], 71), 0),
        "query": draw_query(jax.random.fold_in(key_list[7], 71), 0),
        "key_weight": draw_key_weight(jax.random.fold_in(key_list[7], 71), 0),
        "value_weight": bell_draw(key_list[4], (D, D), D ** -0.5, 0.1875, ((0, 8),)),
        "out_weight": bell_draw(key_list[5], (D, D), D ** -0.5, 0.1875, ((0, 8),)),
        "var_slot": draw_var_slot(jax.random.fold_in(key_list[7], 71), 0),
    }


def reference(tokens, var_embed, query, key_weight, value_weight, out_weight, var_slot):
    head_dim = D // HEADS
    scale = 1.0 / math.sqrt(head_dim)
    query_heads = query.astype(jnp.float32).reshape(HEADS, head_dim)
    embed_float = var_embed.astype(jnp.float32)

    def block(index):
        start = (index * PATCH_DEV).astype(jnp.int32)
        window = lax.dynamic_slice_in_dim(tokens, start, PATCH_DEV, 2)
        selected = jnp.take(window, var_slot.astype(jnp.int32), axis=0)
        mixed = (selected.astype(jnp.float32) + embed_float[:, None, None, :]).astype(jnp.bfloat16)
        flattened = mixed.reshape(-1, D)
        keys = jnp.dot(flattened.astype(jnp.float32), key_weight.astype(jnp.float32), preferred_element_type=jnp.float32).astype(jnp.bfloat16)
        values = jnp.dot(flattened.astype(jnp.float32), value_weight.astype(jnp.float32), preferred_element_type=jnp.float32).astype(jnp.bfloat16)
        keys = keys.reshape(VARS, B, PATCH_DEV, HEADS, head_dim)
        values = values.reshape(VARS, B, PATCH_DEV, HEADS, head_dim)
        scores = jnp.einsum('vbphe,he->vbph', keys.astype(jnp.float32), query_heads) * scale
        highest = lax.optimization_barrier(jnp.max(scores, axis=0, keepdims=True))
        exponent = jnp.exp(scores - highest)
        weights = (exponent / lax.optimization_barrier(jnp.sum(exponent, axis=0, keepdims=True))).astype(jnp.bfloat16)
        context = jnp.einsum('vbph,vbphe->bphe', weights.astype(jnp.float32), values.astype(jnp.float32))
        context = context.astype(jnp.bfloat16).reshape(B * PATCH_DEV, D)
        result = jnp.dot(context.astype(jnp.float32), out_weight.astype(jnp.float32), preferred_element_type=jnp.float32).astype(jnp.bfloat16)
        return result.reshape(B, PATCH_DEV, D)
    blocks = lax.map(block, jnp.arange(PATCH // PATCH_DEV, dtype=jnp.int32))
    return jnp.transpose(blocks, (1, 0, 2, 3)).reshape(B, PATCH, D)
```

```python
import functools
import math

import jax
import jax.numpy as jnp
from jax import lax
from jax.experimental import pallas as pl
from jax.experimental.pallas import tpu as pltpu
from jax.sharding import PartitionSpec as P

HEADS = 16
CORES = 2
CHUNK = 256
LOWEST = -1e38
F32 = jnp.float32
BF16 = jnp.bfloat16
MESH = pl.DeviceIdType.MESH
NT = (((1,), (1,)), ((), ()))


def split(x):
    high = x.astype(BF16)
    return high, (x - high.astype(F32)).astype(BF16)


def dot(a, b):
    return jnp.dot(a, b, preferred_element_type=F32)


def kernel(nx, ny, heads, tok_any, emb_any, qry_any, wk_any, wv_any, wo_any, slot_any, out,
           tok, emb, qry, wk, wo, slot, mixed, wbuf, wother, kq_mine, kq_in, kq_all, ex,
           stat, st_in, st2, st2_in, fexp, part, in1, p2, in2, o3, in3,
           load_s, send_s, kq_r, z_r, w_r, tok_r, st_r, st2_r, s1_r, s2_r, s3_r):
    _, slots, patches, width = tok.shape
    rows = width // ny
    na = ny // CORES
    group = patches // nx
    piece = rows // nx
    lane = width // CORES
    chunk = min(CHUNK, lane)
    chunks = lane // chunk
    per_chunk = chunk // rows
    own = patches // (nx * ny)
    hdim = width // heads
    lheads = heads // CORES
    held_slots = CORES * slots
    block_rows = held_slots * group
    scale = 1.0 / math.sqrt(hdim)
    i = lax.axis_index("vx")
    j = lax.axis_index("vy")
    a = j // CORES
    c = j % CORES
    partner = a * CORES + (1 - c)
    x_peers = [lax.rem(i + d, nx) for d in range(1, nx)]
    a_peers = [lax.rem(a + d, na) for d in range(1, na)]
    vy_peers = [lax.rem(j + d, ny) for d in range(1, ny)]

    def remote(src, dst, rs, x, y):
        return pltpu.make_async_remote_copy(
            src_ref=src, dst_ref=dst, send_sem=send_s, recv_sem=rs,
            device_id=(x, y), device_id_type=MESH)

    sent = []

    def send(*args):
        copy = remote(*args)
        copy.start()
        sent.append(copy)

    def arrived(ref, rs):
        remote(ref, ref, rs, i, j).wait_recv()

    def half(which):
        return wv_any.at[:, pl.ds(pl.multiple_of(which * lane, lane), lane)]

    pairs = ((wk_any, wk), (qry_any, qry), (half(c), wbuf.at[j]), (half(1 - c), wother),
             (tok_any, tok.at[c]), (emb_any, emb), (slot_any, slot), (wo_any, wo))
    loads = [pltpu.make_async_copy(src, dst, load_s.at[n]) for n, (src, dst) in enumerate(pairs)]
    for load in loads:
        load.start()

    barrier = pltpu.get_barrier_semaphore()
    for y in vy_peers:
        pl.semaphore_signal(barrier, inc=1, device_id=(i, y), device_id_type=MESH)
    for x in x_peers:
        pl.semaphore_signal(barrier, inc=1, device_id=(x, j), device_id_type=MESH)

    with jax.named_scope("A_load01"):
        loads[0].wait()
        loads[1].wait()
    head_row = lax.broadcasted_iota(jnp.int32, (heads, width), 0)
    head_col = lax.broadcasted_iota(jnp.int32, (heads, width), 1) // hdim
    qmat = jnp.where(head_row == head_col, jnp.broadcast_to(qry[...].astype(F32).reshape(1, width), (heads, width)), 0.0).astype(BF16)
    kq = lax.dot_general(qmat, wk[...], NT, preferred_element_type=F32)
    for d in range(CORES):
        kq_high, kq_low = split(kq[d * lheads:(d + 1) * lheads])
        kq_mine[d, 0] = kq_high
        kq_mine[d, 1] = kq_low

    with jax.named_scope("B_barrier"):
        pl.semaphore_wait(barrier, (ny - 1) + (nx - 1))

    for y in vy_peers:
        send(kq_mine.at[y % CORES], kq_in.at[j], kq_r, i, y)

    def cols(n):
        return pl.ds(n * chunk, chunk)

    def piece_rows(q):
        return pl.ds(pl.multiple_of(q * piece, piece), piece)

    with jax.named_scope("C_load23"):
        loads[2].wait()
        loads[3].wait()
    for n in range(chunks):
        for x in a_peers:
            here = wbuf.at[j, piece_rows(i), cols(n)]
            send(here, here, z_r.at[n, a], i, x * CORES + c)
            send(wother.at[piece_rows(i), cols(n)], here, z_r.at[n, a], i, x * CORES + (1 - c))
        send(wother.at[:, cols(n)], wbuf.at[j, :, cols(n)], w_r.at[n, a], i, partner)
    with jax.named_scope("C_load4"):
        loads[4].wait()
    send(tok.at[c], tok.at[c], tok_r, i, partner)

    kq_in[j] = kq_mine[c]

    def pair_rows(x, q, n):
        return wbuf.at[pl.ds(pl.multiple_of(x * CORES, CORES), CORES), piece_rows(q), cols(n)]

    def share(n):
        for x in a_peers:
            here = pair_rows(x, i, n)
            arrived(here, z_r.at[n, x])
            for q in x_peers:
                send(here, here, w_r.at[n, x], q, j)

    def complete(n):
        arrived(wbuf.at[partner, :, cols(n)], w_r.at[n, a])
        for x in a_peers:
            arrived(wbuf.at[pl.ds(pl.multiple_of(x * CORES, CORES), CORES), 0:(nx - 1) * piece, cols(n)], w_r.at[n, x])

    with jax.named_scope("D_loads"):
        for load in loads[5:]:
            load.wait()
    count = slot.shape[1]
    padded = -(-held_slots // 8) * 8
    ids = (i * ny + a * CORES) * slots + lax.broadcasted_iota(jnp.int32, (padded, count), 0)
    match = jnp.where(ids == jnp.broadcast_to(slot[...], (padded, count)), 1.0, 0.0)
    held = jnp.max(match, axis=1, keepdims=True)
    embed = dot(match.astype(BF16), emb[...])

    def mix(core):
        for s in range(slots):
            m = core * slots + s
            line = jnp.sum(jnp.where(lax.broadcasted_iota(jnp.int32, (padded, width), 0) == m, embed, 0.0), axis=0, keepdims=True)
            for g in range(nx):
                first = pl.multiple_of(g * block_rows + m * group, group)
                mixed[pl.ds(first, group), :] = (tok[core, s, g * group:(g + 1) * group, :].astype(F32) + line).astype(BF16)

    with jax.named_scope("E_mix"):
        mix(c)
    with jax.named_scope("F_share0"):
        share(0)
    with jax.named_scope("G_tok"):
        arrived(tok.at[1 - c], tok_r)
    with jax.named_scope("G_mix2"):
        mix(1 - c)

    with jax.named_scope("H_kq"):
        arrived(kq_in.at[0:ny - 1], kq_r)
    for y in range(ny):
        for d in range(2):
            kq_all[d * lheads:(d + 1) * lheads, y * rows:(y + 1) * rows] = kq_in[y, d]
    for g in range(nx):
        both = lax.dot_general(mixed[g * block_rows:(g + 1) * block_rows, :], kq_all[...], NT, preferred_element_type=F32)
        score = scale * (both[:, 0:lheads] + both[:, lheads:2 * lheads])
        top = jnp.full((group, lheads), LOWEST, F32)
        scores = []
        for s in range(held_slots):
            here = jnp.where(held[s:s + 1, :] > 0, score[s * group:(s + 1) * group], LOWEST)
            scores.append(here)
            top = jnp.maximum(top, here)
        total = jnp.zeros((group, lheads), F32)
        for s in range(held_slots):
            e = jnp.where(held[s:s + 1, :] > 0, jnp.exp(scores[s] - top), 0.0).astype(BF16)
            ex[g * block_rows + s * group:g * block_rows + (s + 1) * group, :] = e
            total += e.astype(F32)
        stat[g, :, 0:lheads] = top
        stat[g, :, lheads:2 * lheads] = total

    for q in x_peers:
        send(stat.at[q], st_in.at[i], st_r, q, j)
    st_in[i] = stat[i]

    with jax.named_scope("J_share1"):
        for n in range(1, chunks):
            share(n)

    with jax.named_scope("K_st"):
        arrived(st_in.at[0:nx - 1], st_r)
    tops = [st_in[q][:, 0:lheads] for q in range(nx)]
    high = functools.reduce(jnp.maximum, tops)
    st2[:, 0:lheads] = high
    st2[:, lheads:2 * lheads] = sum(
        jnp.exp(tops[q] - high) * st_in[q][:, lheads:2 * lheads] for q in range(nx))
    for x in a_peers:
        send(st2, st2_in.at[a], st2_r, i, x * CORES + c)
    st2_in[a] = st2[...]

    def project(n):
        col = n * chunk + lax.broadcasted_iota(jnp.int32, (lheads, chunk), 1)
        to_cols = jnp.where(col // hdim == lax.broadcasted_iota(jnp.int32, (lheads, chunk), 0), 1.0, 0.0).astype(BF16)
        for g in x_peers + [i]:
            here = pl.ds(pl.multiple_of(g * block_rows, block_rows), block_rows)
            value = dot(mixed[here, :], wbuf[:, :, n * chunk:(n + 1) * chunk].reshape(width, chunk))
            value = value * dot(ex[here, :], to_cols)
            context = sum(value[s * group:(s + 1) * group] for s in range(held_slots)).astype(BF16)
            if g is i:
                in1[n, i] = context
            else:
                part[n, g] = context
                send(part.at[n, g], in1.at[n, i], s1_r.at[n], g, j)

    def combine(n):
        arrived(in1.at[n, 0:nx - 1], s1_r.at[n])
        acc = sum(fexp[q, :, n * chunk:(n + 1) * chunk] * in1[n, q].astype(F32) for q in range(nx))
        for k in range(per_chunk):
            b = n * per_chunk + k
            p2[b] = acc[:, k * rows:(k + 1) * rows].astype(BF16)
            target = c * na + b

            @pl.when(target != j)
            def _():
                remote(p2.at[b], in2.at[a], s2_r, i, target).start()

    with jax.named_scope("L_complete0"):
        complete(0)
    with jax.named_scope("M_project0"):
        project(0)

    with jax.named_scope("N_st2"):
        arrived(st2_in.at[0:na - 1], st2_r)
    highest = functools.reduce(jnp.maximum, [st2_in[p][:, 0:lheads] for p in range(na)])
    whole = sum(jnp.exp(st2_in[p][:, 0:lheads] - highest) * st2_in[p][:, lheads:2 * lheads] for p in range(na))
    feature = lax.broadcasted_iota(jnp.int32, (lheads, lane), 1)
    spread = jnp.where(feature // hdim == lax.broadcasted_iota(jnp.int32, (lheads, lane), 0), 1.0, 0.0).astype(BF16)
    for q in range(nx):
        f_high, f_low = split(jnp.exp(st_in[q][:, 0:lheads] - highest) / whole)
        fexp[q] = dot(f_high, spread) + dot(f_low, spread)

    for n in range(1, chunks):
        with jax.named_scope("O_complete"):
            complete(n)
        with jax.named_scope("P_project"):
            project(n)
        with jax.named_scope("Q_combine0"):
            combine(n - 1)
    with jax.named_scope("R_combine1"):
        combine(chunks - 1)

    mine = j // na == c

    @pl.when(mine)
    def _():
        in2[a] = p2[lax.rem(j, na)]
        arrived(in2.at[0:na - 1], s2_r)

    @pl.when(jnp.logical_not(mine))
    def _():
        arrived(in2, s2_r)

    acc = sum(in2[x].astype(F32) for x in range(na))
    result = dot(acc.astype(BF16), wo[...]).astype(BF16)
    for y in range(ny):
        o3[y] = result[y * own:(y + 1) * own]
    for y in vy_peers:
        send(o3.at[y], in3.at[j], s3_r, i, y)
    final = o3[j].astype(F32)
    with jax.named_scope("T_in3"):
        arrived(in3.at[0:ny - 1], s3_r)
    for y in vy_peers:
        final += in3[y].astype(F32)
    out[...] = final.astype(BF16)
    with jax.named_scope("U_sends"):
        for copy in sent:
            copy.wait_send()
    for b in range(chunks * per_chunk):
        @pl.when(c * na + b != j)
        def _():
            remote(p2.at[b], in2.at[a], s2_r, i, c * na + b).wait_send()


def shards(tokens, var_embed, query, key_weight, value_weight, out_weight, var_slot):
    slots, batch, patches, width = tokens.shape
    nx, ny = lax.axis_size("vx"), lax.axis_size("vy")
    heads = HEADS
    patches = batch * patches
    rows, na, group, own = width // ny, ny // CORES, patches // nx, patches // (nx * ny)
    lane, lheads = width // CORES, heads // CORES
    chunk = min(CHUNK, lane)
    chunks = lane // chunk
    held = CORES * slots * patches
    dma = pltpu.SemaphoreType.DMA
    vmem = pltpu.VMEM
    result = pl.pallas_call(
        functools.partial(kernel, nx, ny, heads),
        out_shape=vmem((own, width), BF16),
        in_specs=[pl.BlockSpec(memory_space=pl.ANY)] * 7,
        out_specs=pl.BlockSpec(memory_space=vmem),
        scratch_shapes=[
            vmem((CORES, slots, patches, width), BF16),
            vmem(var_embed.shape, BF16),
            vmem((width,), BF16),
            vmem((rows, width), BF16),
            vmem((rows, width), BF16),
            vmem((1, var_slot.shape[0]), jnp.int32),
            vmem((held, width), BF16),
            vmem((ny, rows, lane), BF16),
            vmem((rows, lane), BF16),
            vmem((CORES, 2, lheads, rows), BF16),
            vmem((ny, 2, lheads, rows), BF16),
            vmem((2 * lheads, width), BF16),
            vmem((held, lheads), BF16),
            vmem((nx, group, 2 * lheads), F32),
            vmem((nx, group, 2 * lheads), F32),
            vmem((group, 2 * lheads), F32),
            vmem((na, group, 2 * lheads), F32),
            vmem((nx, group, lane), F32),
            vmem((chunks, nx, group, chunk), BF16),
            vmem((chunks, nx, group, chunk), BF16),
            vmem((na, group, rows), BF16),
            vmem((na, group, rows), BF16),
            vmem((ny, own, width), BF16),
            vmem((ny, own, width), BF16),
            dma((8,)), dma, dma, dma((chunks, na)), dma((chunks, na)), dma, dma, dma,
            dma((chunks,)), dma, dma,
        ],
        compiler_params=pltpu.CompilerParams(
            collective_id=0, has_side_effects=True, vmem_limit_bytes=56 * 1024 * 1024),
    )(
        tokens.reshape(slots, patches, width), var_embed, query,
        key_weight, value_weight, out_weight, var_slot.reshape(1, -1),
    )
    return result.reshape(batch, -1, width)


def solution(mesh):
    placed = (
        P(("vx", "vy"), None, None, None),
        P(),
        P(),
        P("vy", None),
        P("vy", None),
        P("vy", None),
        P(),
    )
    return jax.shard_map(
        shards, mesh=mesh, in_specs=placed, out_specs=P(None, ("vx", "vy"), None), check_vma=False
    )
```

```python
import functools
import math

import jax
import jax.numpy as jnp
from jax import lax
from jax.experimental import pallas as pl
from jax.experimental.pallas import tpu as pltpu
from jax.sharding import PartitionSpec as P

HEADS = 16
CORES = 2
CHUNK = 256
LOWEST = -1e38
F32 = jnp.float32
BF16 = jnp.bfloat16
MESH = pl.DeviceIdType.MESH
NT = (((1,), (1,)), ((), ()))


def split(x):
    high = x.astype(BF16)
    return high, (x - high.astype(F32)).astype(BF16)


def dot(a, b):
    return jnp.dot(a, b, preferred_element_type=F32)


def flip(index, mask, size):
    bit = 1
    while bit < size:
        if mask & bit:
            index = index + bit - 2 * bit * (index // bit % 2)
        bit *= 2
    return index


def kernel(nx, ny, heads, tok_any, emb_any, qry_any, wk_any, wv_any, wo_any, slot_any, out,
           tok, emb, qry, wk, wo, slot, mixed, wbuf, wother, kq_mine, kq_in, kq_all, ex,
           stat, st_in, st2, st2_in, fexp, part, in1, p2, in2, o3, in3,
           load_s, send_s, kq_r, z_r, w_r, tok_r, wo_r, st_r, st2_r, s1_r, s2_r, s3_r):
    _, slots, patches, width = tok.shape
    rows = width // ny
    na = ny // CORES
    group = patches // nx
    piece = rows // nx
    lane = width // CORES
    chunk = min(CHUNK, lane)
    chunks = lane // chunk
    wide = CORES * rows
    per_chunk = chunk // wide
    first_plane = na // CORES
    own = patches // (nx * ny)
    hdim = width // heads
    lheads = heads // CORES
    held_slots = CORES * slots
    block_rows = held_slots * group
    scale = 1.0 / math.sqrt(hdim)
    i = lax.axis_index("vx")
    j = lax.axis_index("vy")
    a = j // CORES
    c = j % CORES
    partner = a * CORES + (1 - c)
    x_peers = [flip(i, d, nx) for d in range(1, nx)]
    mirror = x_peers[-1]
    a_peers = [flip(a, d, na) for d in range(1, na)]
    vy_peers = [lax.rem(j + d, ny) for d in range(1, ny)]

    def remote(src, dst, rs, x, y):
        return pltpu.make_async_remote_copy(
            src_ref=src, dst_ref=dst, send_sem=send_s, recv_sem=rs,
            device_id=(x, y), device_id_type=MESH)

    sent = []

    def send(*args):
        copy = remote(*args)
        copy.start()
        sent.append(copy)

    def arrived(ref, rs):
        remote(ref, ref, rs, i, j).wait_recv()

    def half(which):
        return wv_any.at[:, pl.ds(pl.multiple_of(which * lane, lane), lane)]

    pairs = ((wk_any, wk), (qry_any, qry), (half(c), wbuf.at[j]), (half(1 - c), wother),
             (tok_any, tok.at[c]), (emb_any, emb), (slot_any, slot), (wo_any, wo.at[c]))
    loads = [pltpu.make_async_copy(src, dst, load_s.at[n]) for n, (src, dst) in enumerate(pairs)]
    for load in loads:
        load.start()

    barrier = pltpu.get_barrier_semaphore()
    for y in vy_peers:
        pl.semaphore_signal(barrier, inc=1, device_id=(i, y), device_id_type=MESH)
    for x in x_peers:
        pl.semaphore_signal(barrier, inc=1, device_id=(x, j), device_id_type=MESH)

    with jax.named_scope("A_load01"):
        loads[0].wait()
        loads[1].wait()
    head_row = lax.broadcasted_iota(jnp.int32, (heads, width), 0)
    head_col = lax.broadcasted_iota(jnp.int32, (heads, width), 1) // hdim
    qmat = jnp.where(head_row == head_col, jnp.broadcast_to(qry[...].astype(F32).reshape(1, width), (heads, width)), 0.0).astype(BF16)
    kq = lax.dot_general(qmat, wk[...], NT, preferred_element_type=F32)
    for d in range(CORES):
        kq_high, kq_low = split(kq[d * lheads:(d + 1) * lheads])
        kq_mine[d, 0] = kq_high
        kq_mine[d, 1] = kq_low

    with jax.named_scope("B_barrier"):
        pl.semaphore_wait(barrier, (ny - 1) + (nx - 1))

    for y in vy_peers:
        send(kq_mine.at[y % CORES], kq_in.at[j], kq_r, i, y)

    def cols(n):
        return pl.ds(n * chunk, chunk)

    def piece_rows(q):
        return pl.ds(pl.multiple_of(q * piece, piece), piece)

    with jax.named_scope("C_load23"):
        loads[2].wait()
        loads[3].wait()
    def along_z(q, n, sem):
        for x in a_peers:
            here = wbuf.at[j, piece_rows(q), cols(n)]
            send(here, here, sem, i, x * CORES + c)
            send(wother.at[piece_rows(q), cols(n)], here, sem, i, x * CORES + (1 - c))

    for n in range(chunks):
        along_z(i, n, z_r.at[n, a])
        send(wother.at[:, cols(n)], wbuf.at[j, :, cols(n)], w_r.at[n, a], i, partner)
    for n in range(1, chunks):
        along_z(mirror, n, w_r.at[n, a])
    with jax.named_scope("C_load4"):
        loads[4].wait()
    send(tok.at[c], tok.at[c], tok_r, i, partner)

    kq_in[j] = kq_mine[c]

    def pair_rows(x, q, n):
        return wbuf.at[pl.ds(pl.multiple_of(x * CORES, CORES), CORES), piece_rows(q), cols(n)]

    def share(n, x):
        here = pair_rows(x, i, n)
        arrived(here, z_r.at[n, x])
        for q in x_peers if n == 0 else x_peers[:-1]:
            send(here, here, w_r.at[n, x], q, j)

    def complete(n):
        arrived(wbuf.at[partner, :, cols(n)], w_r.at[n, a])
        for x in a_peers:
            arrived(wbuf.at[pl.ds(pl.multiple_of(x * CORES, CORES), CORES), 0:(nx - 1) * piece, cols(n)], w_r.at[n, x])

    with jax.named_scope("D_loads"):
        for load in loads[5:]:
            load.wait()
    count = slot.shape[1]
    padded = -(-held_slots // 8) * 8
    ids = (i * ny + a * CORES) * slots + lax.broadcasted_iota(jnp.int32, (padded, count), 0)
    match = jnp.where(ids == jnp.broadcast_to(slot[...], (padded, count)), 1.0, 0.0)
    held = jnp.max(match, axis=1, keepdims=True)
    embed = dot(match.astype(BF16), emb[...])

    def mix(core):
        for s in range(slots):
            m = core * slots + s
            line = jnp.sum(jnp.where(lax.broadcasted_iota(jnp.int32, (padded, width), 0) == m, embed, 0.0), axis=0, keepdims=True)
            for g in range(nx):
                first = pl.multiple_of(g * block_rows + m * group, group)
                mixed[pl.ds(first, group), :] = (tok[core, s, g * group:(g + 1) * group, :].astype(F32) + line).astype(BF16)

    send(wo.at[c], wo.at[c], wo_r, i, partner)
    with jax.named_scope("E_mix"):
        mix(c)
    with jax.named_scope("F_share00"):
        share(0, a_peers[0])
    with jax.named_scope("G_tok"):
        arrived(tok.at[1 - c], tok_r)
    with jax.named_scope("G_mix2"):
        mix(1 - c)
    with jax.named_scope("G_share01"):
        for x in a_peers[1:-1]:
            share(0, x)
    with jax.named_scope("H_kq"):
        arrived(kq_in.at[0:ny - 1], kq_r)
    for y in range(ny):
        for d in range(2):
            kq_all[d * lheads:(d + 1) * lheads, y * rows:(y + 1) * rows] = kq_in[y, d]
    for g in range(nx):
        both = lax.dot_general(mixed[g * block_rows:(g + 1) * block_rows, :], kq_all[...], NT, preferred_element_type=F32)
        score = scale * (both[:, 0:lheads] + both[:, lheads:2 * lheads])
        top = jnp.full((group, lheads), LOWEST, F32)
        scores = []
        for s in range(held_slots):
            here = jnp.where(held[s:s + 1, :] > 0, score[s * group:(s + 1) * group], LOWEST)
            scores.append(here)
            top = jnp.maximum(top, here)
        total = jnp.zeros((group, lheads), F32)
        for s in range(held_slots):
            e = jnp.where(held[s:s + 1, :] > 0, jnp.exp(scores[s] - top), 0.0).astype(BF16)
            ex[g * block_rows + s * group:g * block_rows + (s + 1) * group, :] = e
            total += e.astype(F32)
        stat[g, :, 0:lheads] = top
        stat[g, :, lheads:2 * lheads] = total

    for q in x_peers:
        send(stat.at[q], st_in.at[i], st_r, q, j)
    st_in[i] = stat[i]

    with jax.named_scope("J_share02"):
        share(0, a_peers[-1])
    with jax.named_scope("J_share1"):
        for n in range(1, chunks):
            for x in a_peers:
                share(n, x)

    def project(n):
        col = n * chunk + lax.broadcasted_iota(jnp.int32, (lheads, chunk), 1)
        to_cols = jnp.where(col // hdim == lax.broadcasted_iota(jnp.int32, (lheads, chunk), 0), 1.0, 0.0).astype(BF16)
        weight = wbuf[:, :, n * chunk:(n + 1) * chunk].reshape(width, chunk)
        for g in range(nx):
            here = slice(g * block_rows, (g + 1) * block_rows)
            value = dot(mixed[here, :], weight) * dot(ex[here, :], to_cols)
            part[n, g] = sum(value[s * group:(s + 1) * group] for s in range(held_slots)).astype(BF16)
        for q in x_peers:
            send(part.at[n, q], in1.at[n, i], s1_r.at[n], q, j)

    def combine(n):
        arrived(in1.at[n, 0:nx - 1], s1_r.at[n])
        here = slice(n * chunk, (n + 1) * chunk)
        acc = fexp[i, :, here] * part[n, i].astype(F32)
        for q in x_peers:
            acc += fexp[q, :, here] * in1[n, q].astype(F32)
        for k in range(per_chunk):
            b = n * per_chunk + k
            block = acc[:, k * wide:(k + 1) * wide]
            for d in range(CORES):
                picked = [block[(x * CORES + d) * own:(x * CORES + d + 1) * own] for x in range(na)]
                p2[b, d] = jnp.concatenate(picked, axis=0).astype(BF16)
                target = (c * first_plane + b) * CORES + d

                @pl.when(target != j)
                def _():
                    remote(p2.at[b, d], in2.at[a], s2_r, i, target).start()

    with jax.named_scope("K_st"):
        arrived(st_in.at[0:nx - 1], st_r)
    tops = [st_in[q][:, 0:lheads] for q in range(nx)]
    high = functools.reduce(jnp.maximum, tops)
    st2[:, 0:lheads] = high
    st2[:, lheads:2 * lheads] = sum(
        jnp.exp(tops[q] - high) * st_in[q][:, lheads:2 * lheads] for q in range(nx))
    for x in a_peers:
        send(st2, st2_in.at[a], st2_r, i, x * CORES + c)
    st2_in[a] = st2[...]

    with jax.named_scope("L_complete0"):
        complete(0)
    with jax.named_scope("M_project0"):
        project(0)

    for n in range(1, chunks):
        with jax.named_scope("O_complete"):
            complete(n)
        with jax.named_scope("P_project"):
            project(n)
    with jax.named_scope("N_st2"):
        arrived(st2_in.at[0:na - 1], st2_r)
    highest = functools.reduce(jnp.maximum, [st2_in[p][:, 0:lheads] for p in range(na)])
    whole = sum(jnp.exp(st2_in[p][:, 0:lheads] - highest) * st2_in[p][:, lheads:2 * lheads] for p in range(na))
    feature = lax.broadcasted_iota(jnp.int32, (lheads, lane), 1)
    spread = jnp.where(feature // hdim == lax.broadcasted_iota(jnp.int32, (lheads, lane), 0), 1.0, 0.0).astype(BF16)
    for q in range(nx):
        f_high, f_low = split(jnp.exp(st_in[q][:, 0:lheads] - highest) / whole)
        fexp[q] = dot(f_high, spread) + dot(f_low, spread)

    for n in range(chunks):
        with jax.named_scope(f"R_combine{n}"):
            combine(n)

    mine = a // first_plane == c

    @pl.when(mine)
    def _():
        in2[a] = p2[lax.rem(a, first_plane), c]
        arrived(in2.at[0:na - 1], s2_r)

    @pl.when(jnp.logical_not(mine))
    def _():
        arrived(in2, s2_r)

    acc = sum(in2[x].astype(F32) for x in range(na))
    arrived(wo.at[1 - c], wo_r)
    result = dot(acc.astype(BF16), wo[...].reshape(wide, width)).astype(BF16)
    for x in range(na):
        o3[x] = result[x * own:(x + 1) * own]
    for x in a_peers:
        send(o3.at[x], in3.at[a], s3_r, i, x * CORES + c)
    final = o3[a].astype(F32)
    with jax.named_scope("T_in3"):
        arrived(in3.at[0:na - 1], s3_r)
    for x in a_peers:
        final += in3[x].astype(F32)
    out[...] = final.astype(BF16)
    with jax.named_scope("U_sends"):
        for copy in sent:
            copy.wait_send()
    for b in range(chunks * per_chunk):
        for d in range(CORES):
            target = (c * first_plane + b) * CORES + d

            @pl.when(target != j)
            def _():
                remote(p2.at[b, d], in2.at[a], s2_r, i, target).wait_send()


def shards(tokens, var_embed, query, key_weight, value_weight, out_weight, var_slot):
    slots, batch, patches, width = tokens.shape
    nx, ny = lax.axis_size("vx"), lax.axis_size("vy")
    heads = HEADS
    patches = batch * patches
    rows, na, group, own = width // ny, ny // CORES, patches // nx, patches // (nx * ny)
    lane, lheads = width // CORES, heads // CORES
    chunk = min(CHUNK, lane)
    chunks = lane // chunk
    held = CORES * slots * patches
    dma = pltpu.SemaphoreType.DMA
    vmem = pltpu.VMEM
    result = pl.pallas_call(
        functools.partial(kernel, nx, ny, heads),
        out_shape=vmem((own, width), BF16),
        in_specs=[pl.BlockSpec(memory_space=pl.ANY)] * 7,
        out_specs=pl.BlockSpec(memory_space=vmem),
        scratch_shapes=[
            vmem((CORES, slots, patches, width), BF16),
            vmem(var_embed.shape, BF16),
            vmem((width,), BF16),
            vmem((rows, width), BF16),
            vmem((CORES, rows, width), BF16),
            vmem((1, var_slot.shape[0]), jnp.int32),
            vmem((held, width), BF16),
            vmem((ny, rows, lane), BF16),
            vmem((rows, lane), BF16),
            vmem((CORES, 2, lheads, rows), BF16),
            vmem((ny, 2, lheads, rows), BF16),
            vmem((2 * lheads, width), BF16),
            vmem((held, lheads), BF16),
            vmem((nx, group, 2 * lheads), F32),
            vmem((nx, group, 2 * lheads), F32),
            vmem((group, 2 * lheads), F32),
            vmem((na, group, 2 * lheads), F32),
            vmem((nx, group, lane), F32),
            vmem((chunks, nx, group, chunk), BF16),
            vmem((chunks, nx, group, chunk), BF16),
            vmem((na // CORES, CORES, na * own, CORES * rows), BF16),
            vmem((na, na * own, CORES * rows), BF16),
            vmem((na, own, width), BF16),
            vmem((na, own, width), BF16),
            dma((8,)), dma, dma, dma((chunks, na)), dma((chunks, na)), dma, dma, dma, dma,
            dma((chunks,)), dma, dma,
        ],
        compiler_params=pltpu.CompilerParams(
            collective_id=0, has_side_effects=True, vmem_limit_bytes=56 * 1024 * 1024),
    )(
        tokens.reshape(slots, patches, width), var_embed, query,
        key_weight, value_weight, out_weight, var_slot.reshape(1, -1),
    )
    return result.reshape(batch, -1, width)


def solution(mesh):
    placed = (
        P(("vx", "vy"), None, None, None),
        P(),
        P(),
        P("vy", None),
        P("vy", None),
        P("vy", None),
        P(),
    )
    return jax.shard_map(
        shards, mesh=mesh, in_specs=placed, out_specs=P(None, ("vx", "vy"), None), check_vma=False
    )
```

```python
import functools
import math

import jax
import jax.numpy as jnp
from jax import lax
from jax.experimental import pallas as pl
from jax.experimental.pallas import tpu as pltpu
from jax.sharding import PartitionSpec as P

HEADS = 16
CORES = 2
LOWEST = -1e38
F32 = jnp.float32
BF16 = jnp.bfloat16
MESH = pl.DeviceIdType.MESH
NT = (((1,), (1,)), ((), ()))
TN = (((0,), (0,)), ((), ()))


def split(x):
    high = x.astype(BF16)
    return high, (x - high.astype(F32)).astype(BF16)


def dot(a, b):
    return jnp.dot(a, b, preferred_element_type=F32)


def pieces(lane):
    return (0, lane // 2), (lane // 2, lane // 2)


def flip(index, mask, size):
    bit = 1
    while bit < size:
        if mask & bit:
            index = index + bit - 2 * bit * (index // bit % 2)
        bit *= 2
    return index


def kernel(nx, ny, heads, tok_any, emb_any, qry_any, wk_any, wv_any, wo_any, slot_any, out,
           tok, emb, qry, wk, wo, slot, mixed, wbuf, wother, kq_mine, kq_in, kq_all, ex,
           stat, st_in, st2, st2_in, fexp, part, in1, p2, in2, o3, in3, early, spread_ex, tall,
           load_s, send_s, kq_r, z_r, w_r, tok_r, wo_r, st_r, st2_r, s1_r, s2_r, s3_r):
    _, slots, patches, width = tok.shape
    rows = width // ny
    na = ny // CORES
    group = patches // nx
    piece = rows // nx
    lane = width // CORES
    starts, sizes = pieces(lane)
    chunks = len(starts)
    wide = CORES * rows
    first_plane = na // CORES
    own = patches // (nx * ny)
    hdim = width // heads
    lheads = heads // CORES
    cheads = lheads // CORES
    held_slots = CORES * slots
    block_rows = held_slots * group
    scale = 1.0 / math.sqrt(hdim)
    i = lax.axis_index("vx")
    j = lax.axis_index("vy")
    a = j // CORES
    c = j % CORES
    partner = a * CORES + (1 - c)
    x_peers = [flip(i, d, nx) for d in reversed(range(1, nx))]
    mirror = x_peers[0]
    a_peers = [flip(a, d, na) for d in range(1, na)]
    vy_peers = [lax.rem(j + d, ny) for d in range(1, ny)]

    def remote(src, dst, rs, x, y):
        return pltpu.make_async_remote_copy(
            src_ref=src, dst_ref=dst, send_sem=send_s, recv_sem=rs,
            device_id=(x, y), device_id_type=MESH)

    sent = []

    def send(*args):
        copy = remote(*args)
        copy.start()
        sent.append(copy)

    def arrived(ref, rs):
        remote(ref, ref, rs, i, j).wait_recv()

    def cols(n):
        return slice(starts[n], starts[n] + sizes[n])

    def quarter(which, n):
        first = (n + which * (2 * CORES - 1 - 2 * n)) * sizes[n]
        return wv_any.at[:, pl.ds(pl.multiple_of(first, sizes[n]), sizes[n])]

    pairs = ((wk_any, wk), (qry_any, qry),
             (quarter(c, 0), wbuf.at[j, :, cols(0)]), (quarter(1 - c, 0), wother.at[:, cols(0)]),
             (quarter(c, 1), wbuf.at[j, :, cols(1)]), (quarter(1 - c, 1), wother.at[:, cols(1)]),
             (tok_any, tok.at[c]), (emb_any, emb), (slot_any, slot), (wo_any, wo.at[c]))
    loads = [pltpu.make_async_copy(src, dst, load_s.at[n]) for n, (src, dst) in enumerate(pairs)]
    for load in loads:
        load.start()

    barrier = pltpu.get_barrier_semaphore()
    for y in vy_peers:
        pl.semaphore_signal(barrier, inc=1, device_id=(i, y), device_id_type=MESH)
    for x in x_peers:
        pl.semaphore_signal(barrier, inc=1, device_id=(x, j), device_id_type=MESH)

    with jax.named_scope("A_load01"):
        loads[0].wait()
        loads[1].wait()
    head_row = lax.broadcasted_iota(jnp.int32, (heads, width), 0)
    head_col = lax.broadcasted_iota(jnp.int32, (heads, width), 1) // hdim
    qmat = jnp.where(head_row == head_col, jnp.broadcast_to(qry[...].astype(F32).reshape(1, width), (heads, width)), 0.0).astype(BF16)
    kq = lax.dot_general(qmat, wk[...], NT, preferred_element_type=F32)
    for d in range(CORES):
        for n in range(CORES):
            first = (n if d == 0 else 2 * CORES - 1 - n) * cheads
            kq_high, kq_low = split(kq[first:first + cheads])
            kq_mine[d, 0, n * cheads:(n + 1) * cheads] = kq_high
            kq_mine[d, 1, n * cheads:(n + 1) * cheads] = kq_low

    with jax.named_scope("B_barrier"):
        pl.semaphore_wait(barrier, (ny - 1) + (nx - 1))

    for y in vy_peers:
        send(kq_mine.at[y % CORES], kq_in.at[j], kq_r, i, y)

    def piece_rows(q):
        return pl.ds(pl.multiple_of(q * piece, piece), piece)

    with jax.named_scope("C_load23"):
        for load in loads[2:6]:
            load.wait()
    def along_z(q, n, x, sem):
        here = wbuf.at[j, piece_rows(q), cols(n)]
        send(here, here, sem, i, x * CORES + c)
        send(wother.at[piece_rows(q), cols(n)], here, sem, i, x * CORES + (1 - c))

    for n in range(chunks):
        for x in a_peers:
            along_z(i, n, x, z_r.at[n, a])
        if n == 0:
            along_z(mirror, n, a_peers[0], w_r.at[n, a])
        send(wother.at[:, cols(n)], wbuf.at[j, :, cols(n)], w_r.at[n, a], i, partner)
    with jax.named_scope("C_load4"):
        loads[6].wait()
    send(tok.at[c], tok.at[c], tok_r, i, partner)

    kq_in[j] = kq_mine[c]

    def pair_rows(x, q, n):
        return wbuf.at[pl.ds(pl.multiple_of(x * CORES, CORES), CORES), piece_rows(q), cols(n)]

    def share(n, x):
        here = pair_rows(x, i, n)
        arrived(here, z_r.at[n, x])
        for q in x_peers[1:] if n > 0 or x is a_peers[0] else x_peers:
            send(here, here, w_r.at[n, x], q, j)

    def complete(n, sources):
        for x in sources:
            if x is a:
                arrived(wbuf.at[partner, :, cols(n)], w_r.at[n, a])
            else:
                arrived(wbuf.at[pl.ds(pl.multiple_of(x * CORES, CORES), CORES), 0:(nx - 1) * piece, cols(n)], w_r.at[n, x])

    with jax.named_scope("D_loads"):
        for load in loads[7:]:
            load.wait()
    count = slot.shape[1]
    padded = -(-held_slots // 8) * 8
    ids = (i * ny + a * CORES) * slots + lax.broadcasted_iota(jnp.int32, (padded, count), 0)
    match = jnp.where(ids == jnp.broadcast_to(slot[...], (padded, count)), 1.0, 0.0)
    held = jnp.max(match, axis=1, keepdims=True)
    embed = dot(match.astype(BF16), emb[...])

    def mix(core):
        for s in range(slots):
            m = core * slots + s
            line = jnp.sum(jnp.where(lax.broadcasted_iota(jnp.int32, (padded, width), 0) == m, embed, 0.0), axis=0, keepdims=True)
            for g in range(nx):
                first = pl.multiple_of(g * block_rows + m * group, group)
                mixed[pl.ds(first, group), :] = (tok[core, s, g * group:(g + 1) * group, :].astype(F32) + line).astype(BF16)

    send(wo.at[c], wo.at[c], wo_r, i, partner)
    with jax.named_scope("E_mix"):
        mix(c)
    with jax.named_scope("F_share00"):
        share(0, a_peers[0])
    with jax.named_scope("G_tok"):
        arrived(tok.at[1 - c], tok_r)
    with jax.named_scope("G_mix2"):
        mix(1 - c)
    with jax.named_scope("G_share01"):
        for x in a_peers[1:-1]:
            share(0, x)
    for n in range(1, chunks):
        for x in a_peers:
            along_z(mirror, n, x, w_r.at[n, a])
    with jax.named_scope("J_share02"):
        share(0, a_peers[-1])
    with jax.named_scope("H_kq"):
        arrived(kq_in.at[0:ny - 1], kq_r)
    for y in range(ny):
        for d in range(2):
            kq_all[d * lheads:(d + 1) * lheads, y * rows:(y + 1) * rows] = kq_in[y, d]
    for g in range(nx):
        both = lax.dot_general(mixed[g * block_rows:(g + 1) * block_rows, :], kq_all[...], NT, preferred_element_type=F32)
        score = scale * (both[:, 0:lheads] + both[:, lheads:2 * lheads])
        top = jnp.full((group, lheads), LOWEST, F32)
        scores = []
        for s in range(held_slots):
            here = jnp.where(held[s:s + 1, :] > 0, score[s * group:(s + 1) * group], LOWEST)
            scores.append(here)
            top = jnp.maximum(top, here)
        total = jnp.zeros((group, lheads), F32)
        for s in range(held_slots):
            e = jnp.where(held[s:s + 1, :] > 0, jnp.exp(scores[s] - top), 0.0).astype(BF16)
            ex[g * block_rows + s * group:g * block_rows + (s + 1) * group, :] = e
            total += e.astype(F32)
        tall[g * group:(g + 1) * group, 0:lheads] = top
        tall[g * group:(g + 1) * group, lheads:2 * lheads] = total
    flat = tall[...].T
    for g in range(nx):
        for d in range(CORES):
            for k in range(2):
                first = k * lheads + d * cheads
                stat[g, d, k * cheads:(k + 1) * cheads] = flat[first:first + cheads, g * group:(g + 1) * group]

    for q in x_peers:
        for d in range(CORES):
            send(stat.at[q, d], st_in.at[i * CORES + c], st_r, q, a * CORES + d)
    send(stat.at[i, 1 - c], st_in.at[i * CORES + c], st_r, i, partner)
    st_in[i * CORES + c] = stat[i, c]

    with jax.named_scope("J_share1"):
        for n in range(1, chunks):
            for x in a_peers:
                share(n, x)

    def group_rows(g):
        return slice(g * block_rows, (g + 1) * block_rows)

    feature = lax.broadcasted_iota(jnp.int32, (lheads, lane), 1)
    spread = jnp.where(feature // hdim == lax.broadcasted_iota(jnp.int32, (lheads, lane), 0), 1.0, 0.0).astype(BF16)

    def plane_product(x, here, where):
        first = pl.multiple_of(x * wide, wide)
        weight = wbuf[pl.ds(pl.multiple_of(x * CORES, CORES), CORES), :, where].reshape(wide, -1)
        return dot(mixed[here, pl.ds(first, wide)], weight)

    def project_early(n, sources):
        for g in range(nx):
            here = group_rows(g)
            early[here, cols(n)] = sum(plane_product(x, here, cols(n)) for x in sources)

    def project_late(n, sources):
        for g in range(nx):
            here = group_rows(g)
            value = sum(plane_product(x, here, cols(n)) for x in sources)
            value = (value + early[here, cols(n)]) * spread_ex[here, cols(n)]
            part[n, g] = sum(value[s * group:(s + 1) * group] for s in range(held_slots)).astype(BF16)
        for q in x_peers:
            send(part.at[n, q], in1.at[i * CORES + c], s1_r, q, a * CORES + n)

        @pl.when(c == n)
        def _():
            in1[i * CORES + c] = part[n, i]

        @pl.when(c != n)
        def _():
            remote(part.at[n, i], in1.at[i * CORES + c], s1_r, i, partner).start()

    half_planes = first_plane // CORES
    targets = [(d, k) for d in range(CORES) for k in range(half_planes)]

    def target_of(d, k, core):
        return (c * half_planes + k if d == 0 else na - (c + 1) * half_planes + k) * CORES + core

    def scatter(d, k, core):
        return remote(p2.at[d * half_planes + k, core], in2.at[a], s2_r, i, target_of(d, k, core))

    def combine():
        arrived(in1.at[0:nx * CORES - 1], s1_r)
        for d in range(CORES):
            acc = sum(fexp[q, :, cols(d)] * in1[q * CORES + d].astype(F32) for q in range(nx))
            for k in range(half_planes):
                block = acc[:, k * wide:(k + 1) * wide]
                for core in range(CORES):
                    picked = [block[(x * CORES + core) * own:(x * CORES + core + 1) * own] for x in range(na)]
                    p2[d * half_planes + k, core] = jnp.concatenate(picked, axis=0).astype(BF16)
                    far = target_of(d, k, core) != j

                    @pl.when(far)
                    def _():
                        scatter(d, k, core).start()

    spread_ex[...] = dot(ex[...], spread)
    with jax.named_scope("K_complete0"):
        complete(0, [a] + a_peers[:-2])
    with jax.named_scope("K_early0"):
        project_early(0, [a] + a_peers[:-2])
    with jax.named_scope("L_complete0"):
        complete(0, a_peers[-2:])
    with jax.named_scope("M_project0"):
        project_late(0, a_peers[-2:])
    with jax.named_scope("K_st"):
        arrived(st_in.at[0:nx * CORES - 1], st_r)
    tops = [jnp.concatenate([st_in[q * CORES + d, 0:cheads] for d in range(CORES)], axis=0) for q in range(nx)]
    totals = [jnp.concatenate([st_in[q * CORES + d, cheads:2 * cheads] for d in range(CORES)], axis=0) for q in range(nx)]
    high = functools.reduce(jnp.maximum, tops)
    st2[0:lheads] = high
    st2[lheads:2 * lheads] = sum(
        jnp.exp(tops[q] - high) * totals[q] for q in range(nx))
    for x in a_peers:
        send(st2, st2_in.at[a], st2_r, i, x * CORES + c)
    st2_in[a] = st2[...]
    for n in range(1, chunks):
        with jax.named_scope("O_early1"):
            complete(n, [a])
            project_early(n, [a])
        with jax.named_scope("O_complete1"):
            complete(n, a_peers)
        with jax.named_scope("P_project1"):
            project_late(n, a_peers)
    with jax.named_scope("N_st2"):
        arrived(st2_in.at[0:na - 1], st2_r)
    highest = functools.reduce(jnp.maximum, [st2_in[p, 0:lheads] for p in range(na)])
    whole = sum(jnp.exp(st2_in[p, 0:lheads] - highest) * st2_in[p, lheads:2 * lheads] for p in range(na))
    for q in range(nx):
        f_high, f_low = split(jnp.exp(tops[q] - highest) / whole)
        fexp[q] = (lax.dot_general(f_high, spread, TN, preferred_element_type=F32)
                   + lax.dot_general(f_low, spread, TN, preferred_element_type=F32))

    with jax.named_scope("R_combine1"):
        combine()

    side = a // first_plane
    mine = (a + side * (na - 1 - 2 * a)) // half_planes == c

    @pl.when(mine)
    def _():
        in2[a] = p2[side * half_planes + lax.rem(a, half_planes), c]
        arrived(in2.at[0:na - 1], s2_r)

    @pl.when(jnp.logical_not(mine))
    def _():
        arrived(in2, s2_r)

    acc = sum(in2[x].astype(F32) for x in range(na))
    arrived(wo.at[1 - c], wo_r)
    result = dot(acc.astype(BF16), wo[...].reshape(wide, width)).astype(BF16)
    for x in range(na):
        o3[x] = result[x * own:(x + 1) * own]
    for x in a_peers:
        send(o3.at[x], in3.at[a], s3_r, i, x * CORES + c)
    final = o3[a].astype(F32)
    with jax.named_scope("T_in3"):
        arrived(in3.at[0:na - 1], s3_r)
    for x in a_peers:
        final += in3[x].astype(F32)
    out[...] = final.astype(BF16)
    with jax.named_scope("U_sends"):
        for copy in sent:
            copy.wait_send()
    for n in range(chunks):
        @pl.when(c != n)
        def _():
            remote(part.at[n, i], in1.at[i * CORES + c], s1_r, i, partner).wait_send()
    for d, k in targets:
        for core in range(CORES):
            @pl.when(target_of(d, k, core) != j)
            def _():
                scatter(d, k, core).wait_send()


def shards(tokens, var_embed, query, key_weight, value_weight, out_weight, var_slot):
    slots, batch, patches, width = tokens.shape
    nx, ny = lax.axis_size("vx"), lax.axis_size("vy")
    heads = HEADS
    patches = batch * patches
    rows, na, group, own = width // ny, ny // CORES, patches // nx, patches // (nx * ny)
    lane, lheads = width // CORES, heads // CORES
    chunks = len(pieces(lane)[0])
    held = CORES * slots * patches
    dma = pltpu.SemaphoreType.DMA
    vmem = pltpu.VMEM
    result = pl.pallas_call(
        functools.partial(kernel, nx, ny, heads),
        out_shape=vmem((own, width), BF16),
        in_specs=[pl.BlockSpec(memory_space=pl.ANY)] * 7,
        out_specs=pl.BlockSpec(memory_space=vmem),
        scratch_shapes=[
            vmem((CORES, slots, patches, width), BF16),
            vmem(var_embed.shape, BF16),
            vmem((width,), BF16),
            vmem((rows, width), BF16),
            vmem((CORES, rows, width), BF16),
            vmem((1, var_slot.shape[0]), jnp.int32),
            vmem((held, width), BF16),
            vmem((ny, rows, lane), BF16),
            vmem((rows, lane), BF16),
            vmem((CORES, 2, lheads, rows), BF16),
            vmem((ny, 2, lheads, rows), BF16),
            vmem((2 * lheads, width), BF16),
            vmem((held, lheads), BF16),
            vmem((nx, CORES, lheads, group), F32),
            vmem((nx * CORES, lheads, group), F32),
            vmem((2 * lheads, group), F32),
            vmem((na, 2 * lheads, group), F32),
            vmem((nx, group, lane), F32),
            vmem((chunks, nx, group, lane // chunks), BF16),
            vmem((nx * CORES, group, lane // chunks), BF16),
            vmem((na // CORES, CORES, na * own, CORES * rows), BF16),
            vmem((na, na * own, CORES * rows), BF16),
            vmem((na, own, width), BF16),
            vmem((na, own, width), BF16),
            vmem((held, lane), F32),
            vmem((held, lane), F32),
            vmem((patches, 128), F32),
            dma((10,)), dma, dma, dma((chunks, na)), dma((chunks, na)), dma, dma, dma, dma,
            dma, dma, dma,
        ],
        compiler_params=pltpu.CompilerParams(
            collective_id=0, has_side_effects=True, vmem_limit_bytes=56 * 1024 * 1024),
    )(
        tokens.reshape(slots, patches, width), var_embed, query,
        key_weight, value_weight, out_weight, var_slot.reshape(1, -1),
    )
    return result.reshape(batch, -1, width)


def solution(mesh):
    placed = (
        P(("vx", "vy"), None, None, None),
        P(),
        P(),
        P("vy", None),
        P("vy", None),
        P("vy", None),
        P(),
    )
    return jax.shard_map(
        shards, mesh=mesh, in_specs=placed, out_specs=P(None, ("vx", "vy"), None), check_vma=False
    )
```

```python
import functools
import math

import jax
import jax.numpy as jnp
from jax import lax
from jax.experimental import pallas as pl
from jax.experimental.pallas import tpu as pltpu
from jax.sharding import PartitionSpec as P

HEADS = 16
CORES = 2
LOWEST = -1e38
F32 = jnp.float32
BF16 = jnp.bfloat16
MESH = pl.DeviceIdType.MESH
NT = (((1,), (1,)), ((), ()))
TN = (((0,), (0,)), ((), ()))


def split(x):
    high = x.astype(BF16)
    return high, (x - high.astype(F32)).astype(BF16)


def dot(a, b):
    return jnp.dot(a, b, preferred_element_type=F32)


def pieces(lane):
    return (0, lane // 2), (lane // 2, lane // 2)


def flip(index, mask, size):
    bit = 1
    while bit < size:
        if mask & bit:
            index = index + bit - 2 * bit * (index // bit % 2)
        bit *= 2
    return index


def kernel(nx, ny, heads, tok_any, emb_any, qry_any, wk_any, wv_any, wo_any, slot_any, out,
           tok, emb, qry, wk, wo, slot, mixed, wbuf, wother, kq_mine, kq_in, kq_all, ex,
           stat, st_in, st2, st2_in, fexp, part, in1, p2, in2, o3, in3, early, spread_ex, tall, fz,
           load_s, send_s, kq_r, z_r, w_r, tok_r, wo_r, st_r, st2_r, s1_r, s2_r, s3_r):
    _, slots, patches, width = tok.shape
    rows = width // ny
    na = ny // CORES
    group = patches // nx
    piece = rows // nx
    lane = width // CORES
    starts, sizes = pieces(lane)
    chunks = len(starts)
    wide = CORES * rows
    first_plane = na // CORES
    own = patches // (nx * ny)
    hdim = width // heads
    lheads = heads // CORES
    cheads = lheads // CORES
    held_slots = CORES * slots
    block_rows = held_slots * group
    scale = 1.0 / math.sqrt(hdim)
    i = lax.axis_index("vx")
    j = lax.axis_index("vy")
    a = j // CORES
    c = j % CORES
    partner = a * CORES + (1 - c)
    x_peers = [flip(i, d, nx) for d in reversed(range(1, nx))]
    mirror = x_peers[0]
    a_peers = [flip(a, d, na) for d in range(1, na)]
    vy_peers = [lax.rem(j + d, ny) for d in range(1, ny)]

    def remote(src, dst, rs, x, y):
        return pltpu.make_async_remote_copy(
            src_ref=src, dst_ref=dst, send_sem=send_s, recv_sem=rs,
            device_id=(x, y), device_id_type=MESH)

    sent = []

    def send(*args):
        copy = remote(*args)
        copy.start()
        sent.append(copy)

    def arrived(ref, rs):
        remote(ref, ref, rs, i, j).wait_recv()

    barrier = pltpu.get_barrier_semaphore()
    for y in vy_peers:
        pl.semaphore_signal(barrier, inc=1, device_id=(i, y), device_id_type=MESH)
    for x in x_peers:
        pl.semaphore_signal(barrier, inc=1, device_id=(x, j), device_id_type=MESH)

    def cols(n):
        return slice(starts[n], starts[n] + sizes[n])

    def quarter(which, n):
        first = (n + which * (2 * CORES - 1 - 2 * n)) * sizes[n]
        return wv_any.at[:, pl.ds(pl.multiple_of(first, sizes[n]), sizes[n])]

    pairs = ((wk_any, wk), (qry_any, qry),
             (quarter(c, 0), wbuf.at[j, :, cols(0)]), (quarter(1 - c, 0), wother.at[:, cols(0)]),
             (quarter(c, 1), wbuf.at[j, :, cols(1)]), (quarter(1 - c, 1), wother.at[:, cols(1)]),
             (tok_any, tok.at[c]), (emb_any, emb), (slot_any, slot), (wo_any, wo.at[c]))
    loads = [pltpu.make_async_copy(src, dst, load_s.at[n]) for n, (src, dst) in enumerate(pairs)]
    for load in loads:
        load.start()

    with jax.named_scope("A_load01"):
        loads[0].wait()
        loads[1].wait()
    head_row = lax.broadcasted_iota(jnp.int32, (heads, width), 0)
    head_col = lax.broadcasted_iota(jnp.int32, (heads, width), 1) // hdim
    qmat = jnp.where(head_row == head_col, jnp.broadcast_to(qry[...].astype(F32).reshape(1, width), (heads, width)), 0.0).astype(BF16)
    kq = lax.dot_general(qmat, wk[...], NT, preferred_element_type=F32)
    for d in range(CORES):
        for n in range(CORES):
            first = (n if d == 0 else 2 * CORES - 1 - n) * cheads
            kq_high, kq_low = split(kq[first:first + cheads])
            kq_mine[d, 0, n * cheads:(n + 1) * cheads] = kq_high
            kq_mine[d, 1, n * cheads:(n + 1) * cheads] = kq_low

    with jax.named_scope("B_barrier"):
        pl.semaphore_wait(barrier, (ny - 1) + (nx - 1))

    for y in vy_peers:
        send(kq_mine.at[y % CORES], kq_in.at[j], kq_r, i, y)

    def piece_rows(q):
        return pl.ds(pl.multiple_of(q * piece, piece), piece)

    with jax.named_scope("C_load23"):
        for load in loads[2:6]:
            load.wait()
    def along_z(q, n, x, sem):
        here = wbuf.at[j, piece_rows(q), cols(n)]
        send(here, here, sem, i, x * CORES + c)
        send(wother.at[piece_rows(q), cols(n)], here, sem, i, x * CORES + (1 - c))

    for n in range(chunks):
        for x in a_peers:
            along_z(i, n, x, z_r.at[n, a])
        if n == 0:
            along_z(mirror, n, a_peers[0], w_r.at[n, a])
        send(wother.at[:, cols(n)], wbuf.at[j, :, cols(n)], w_r.at[n, a], i, partner)
    with jax.named_scope("C_load4"):
        loads[6].wait()
    send(tok.at[c], tok.at[c], tok_r, i, partner)

    kq_in[j] = kq_mine[c]

    def pair_rows(x, q, n):
        return wbuf.at[pl.ds(pl.multiple_of(x * CORES, CORES), CORES), piece_rows(q), cols(n)]

    def share(n, x):
        here = pair_rows(x, i, n)
        arrived(here, z_r.at[n, x])
        for q in x_peers[1:] if n > 0 or x is a_peers[0] else x_peers:
            send(here, here, w_r.at[n, x], q, j)

    def complete(n, sources):
        for x in sources:
            if x is a:
                arrived(wbuf.at[partner, :, cols(n)], w_r.at[n, a])
            else:
                arrived(wbuf.at[pl.ds(pl.multiple_of(x * CORES, CORES), CORES), 0:(nx - 1) * piece, cols(n)], w_r.at[n, x])

    with jax.named_scope("D_loads"):
        for load in loads[7:]:
            load.wait()
    count = slot.shape[1]
    padded = -(-held_slots // 8) * 8
    ids = (i * ny + a * CORES) * slots + lax.broadcasted_iota(jnp.int32, (padded, count), 0)
    match = jnp.where(ids == jnp.broadcast_to(slot[...], (padded, count)), 1.0, 0.0)
    held = jnp.max(match, axis=1, keepdims=True)
    embed = dot(match.astype(BF16), emb[...])

    def mix(core):
        for s in range(slots):
            m = core * slots + s
            line = jnp.sum(jnp.where(lax.broadcasted_iota(jnp.int32, (padded, width), 0) == m, embed, 0.0), axis=0, keepdims=True)
            for g in range(nx):
                first = pl.multiple_of(g * block_rows + m * group, group)
                mixed[pl.ds(first, group), :] = (tok[core, s, g * group:(g + 1) * group, :].astype(F32) + line).astype(BF16)

    lend = remote(wo.at[0], wo.at[0], wo_r, i, partner)

    @pl.when(c == 0)
    def _():
        lend.start()

    with jax.named_scope("E_mix"):
        mix(c)
    with jax.named_scope("F_share00"):
        share(0, a_peers[0])
    with jax.named_scope("G_tok"):
        arrived(tok.at[1 - c], tok_r)
    with jax.named_scope("G_mix2"):
        mix(1 - c)
    with jax.named_scope("G_share01"):
        for x in a_peers[1:-1]:
            share(0, x)
    for n in range(1, chunks):
        for x in a_peers:
            along_z(mirror, n, x, w_r.at[n, a])
    with jax.named_scope("J_share02"):
        share(0, a_peers[-1])
    with jax.named_scope("H_kq"):
        arrived(kq_in.at[0:ny - 1], kq_r)
    for y in range(ny):
        for d in range(2):
            kq_all[d * lheads:(d + 1) * lheads, y * rows:(y + 1) * rows] = kq_in[y, d]
    for g in range(nx):
        both = lax.dot_general(mixed[g * block_rows:(g + 1) * block_rows, :], kq_all[...], NT, preferred_element_type=F32)
        score = scale * (both[:, 0:lheads] + both[:, lheads:2 * lheads])
        top = jnp.full((group, lheads), LOWEST, F32)
        scores = []
        for s in range(held_slots):
            here = jnp.where(held[s:s + 1, :] > 0, score[s * group:(s + 1) * group], LOWEST)
            scores.append(here)
            top = jnp.maximum(top, here)
        total = jnp.zeros((group, lheads), F32)
        for s in range(held_slots):
            e = jnp.where(held[s:s + 1, :] > 0, jnp.exp(scores[s] - top), 0.0).astype(BF16)
            ex[g * block_rows + s * group:g * block_rows + (s + 1) * group, :] = e
            total += e.astype(F32)
        tall[g * group:(g + 1) * group, 0:lheads] = top
        tall[g * group:(g + 1) * group, lheads:2 * lheads] = total
    flat = tall[...].T
    for g in range(nx):
        for d in range(CORES):
            for k in range(2):
                first = k * lheads + d * cheads
                stat[g, d, k * cheads:(k + 1) * cheads] = flat[first:first + cheads, g * group:(g + 1) * group]

    for q in x_peers:
        for d in range(CORES):
            send(stat.at[q, d], st_in.at[i * CORES + c], st_r, q, a * CORES + d)
    send(stat.at[i, 1 - c], st_in.at[i * CORES + c], st_r, i, partner)
    st_in[i * CORES + c] = stat[i, c]

    with jax.named_scope("J_share1"):
        for n in range(1, chunks):
            for x in a_peers:
                share(n, x)

    def group_rows(g):
        return slice(g * block_rows, (g + 1) * block_rows)

    feature = lax.broadcasted_iota(jnp.int32, (lheads, lane), 1)
    spread = jnp.where(feature // hdim == lax.broadcasted_iota(jnp.int32, (lheads, lane), 0), 1.0, 0.0).astype(BF16)

    def plane_product(x, here, where):
        first = pl.multiple_of(x * wide, wide)
        weight = wbuf[pl.ds(pl.multiple_of(x * CORES, CORES), CORES), :, where].reshape(wide, -1)
        return dot(mixed[here, pl.ds(first, wide)], weight)

    def project_early(n, sources):
        for g in range(nx):
            here = group_rows(g)
            early[here, cols(n)] = sum(plane_product(x, here, cols(n)) for x in sources)

    def project_late(n, sources):
        near = nx // 2 - 1
        for batch in (x_peers[:near] + [i], x_peers[near:]):
            for g in batch:
                here = pl.ds(pl.multiple_of(g * block_rows, block_rows), block_rows)
                value = sum(plane_product(x, here, cols(n)) for x in sources)
                value = (value + early[here, cols(n)]) * spread_ex[here, cols(n)]
                part[n, g] = sum(value[s * group:(s + 1) * group] for s in range(held_slots)).astype(BF16)
            for g in batch:
                if g is not i:
                    send(part.at[n, g], in1.at[i * CORES + c], s1_r, g, a * CORES + n)

        @pl.when(c == n)
        def _():
            in1[i * CORES + c] = part[n, i]

        @pl.when(c != n)
        def _():
            remote(part.at[n, i], in1.at[i * CORES + c], s1_r, i, partner).start()

    half_planes = first_plane // CORES
    targets = [(d, k) for d in range(CORES) for k in range(half_planes)]

    def target_of(d, k):
        return (c * half_planes + k if d == 0 else na - (c + 1) * half_planes + k) * CORES + CORES - 1

    def scatter(d, k):
        return remote(p2.at[d * half_planes + k], in2.at[a], s2_r, i, target_of(d, k))

    def scatter_stats(d, k):
        return remote(st2.at[d], st2_in.at[a], st2_r, i, target_of(d, k))

    def combine():
        arrived(in1.at[0:nx * CORES - 1], s1_r)
        for d in range(CORES):
            acc = sum(fexp[q, :, cols(d)] * in1[q * CORES + d].astype(F32) for q in range(nx))
            for k in range(half_planes):
                p2[d * half_planes + k] = acc[:, k * wide:(k + 1) * wide].astype(BF16)

                @pl.when(target_of(d, k) != j)
                def _():
                    scatter(d, k).start()

    spread_ex[...] = dot(ex[...], spread)
    with jax.named_scope("K_complete0"):
        complete(0, [a] + a_peers[:-2])
    with jax.named_scope("K_early0"):
        project_early(0, [a] + a_peers[:-2])
    with jax.named_scope("L_complete0"):
        complete(0, a_peers[-2:])
    with jax.named_scope("M_project0"):
        project_late(0, a_peers[-2:])
    with jax.named_scope("K_st"):
        arrived(st_in.at[0:nx * CORES - 1], st_r)
    tops = [jnp.concatenate([st_in[q * CORES + d, 0:cheads] for d in range(CORES)], axis=0) for q in range(nx)]
    totals = [jnp.concatenate([st_in[q * CORES + d, cheads:2 * cheads] for d in range(CORES)], axis=0) for q in range(nx)]
    high = functools.reduce(jnp.maximum, tops)
    below = [jnp.exp(tops[q] - high) for q in range(nx)]
    total = sum(below[q] * totals[q] for q in range(nx))
    for d in range(CORES):
        st2[d, 0:cheads] = high[d * cheads:(d + 1) * cheads]
        st2[d, cheads:lheads] = total[d * cheads:(d + 1) * cheads]
    for d, k in targets:
        @pl.when(target_of(d, k) != j)
        def _():
            scatter_stats(d, k).start()

    for q in range(nx):
        f_high, f_low = split(below[q])
        fexp[q] = (lax.dot_general(f_high, spread, TN, preferred_element_type=F32)
                   + lax.dot_general(f_low, spread, TN, preferred_element_type=F32))

    for n in range(1, chunks):
        with jax.named_scope("O_early1"):
            complete(n, [a])
            project_early(n, [a])
        with jax.named_scope("O_complete1"):
            complete(n, a_peers)
        with jax.named_scope("P_project1"):
            project_late(n, a_peers)
    with jax.named_scope("R_combine1"):
        combine()

    side = a // first_plane
    spot = lax.rem(a, half_planes)
    mine = (a + side * (na - 1 - 2 * a)) // half_planes == CORES - 1

    @pl.when(c == CORES - 1)
    def _():
        @pl.when(mine)
        def _():
            st2_in[a] = st2[side]
            in2[a] = p2[side * half_planes + spot]
            arrived(st2_in.at[0:na - 1], st2_r)

        @pl.when(jnp.logical_not(mine))
        def _():
            arrived(st2_in, st2_r)

        highest = functools.reduce(jnp.maximum, [st2_in[p, 0:cheads] for p in range(na)])
        lower = [jnp.exp(st2_in[p, 0:cheads] - highest) for p in range(na)]
        whole = sum(lower[p] * st2_in[p, cheads:lheads] for p in range(na))
        wanted = (spot * wide + lax.broadcasted_iota(jnp.int32, (cheads, wide), 1)) // hdim
        widen = jnp.where(wanted == lax.broadcasted_iota(jnp.int32, (cheads, wide), 0), 1.0, 0.0).astype(BF16)
        for p in range(na):
            f_high, f_low = split(lower[p] / whole)
            fz[p] = (lax.dot_general(f_high, widen, TN, preferred_element_type=F32)
                     + lax.dot_general(f_low, widen, TN, preferred_element_type=F32))
        arrived(wo.at[0], wo_r)

        with jax.named_scope("S_in2"):
            @pl.when(mine)
            def _():
                arrived(in2.at[0:na - 1], s2_r)

            @pl.when(jnp.logical_not(mine))
            def _():
                arrived(in2, s2_r)

        acc = sum(fz[p] * in2[p].astype(F32) for p in range(na))
        result = dot(acc.astype(BF16), wo[...].reshape(wide, width)).astype(BF16)
        for y in range(ny):
            o3[y] = result[y * own:(y + 1) * own]
        for x in reversed(a_peers):
            for d in range(CORES):
                remote(o3.at[x * CORES + d], in3.at[a], s3_r, i, x * CORES + d).start()
        remote(o3.at[partner], in3.at[a], s3_r, i, partner).start()
        in3[a] = o3[j]
        with jax.named_scope("T_in3n"):
            arrived(in3.at[0:na - 1], s3_r)

    @pl.when(c != CORES - 1)
    def _():
        with jax.named_scope("T_in3s"):
            arrived(in3, s3_r)

    final = sum(in3[x].astype(F32) for x in range(na))
    out[...] = final.astype(BF16)
    with jax.named_scope("U_sends"):
        for copy in sent:
            copy.wait_send()
    for n in range(chunks):
        @pl.when(c != n)
        def _():
            remote(part.at[n, i], in1.at[i * CORES + c], s1_r, i, partner).wait_send()
    for d, k in targets:
        @pl.when(target_of(d, k) != j)
        def _():
            scatter(d, k).wait_send()
            scatter_stats(d, k).wait_send()

    @pl.when(c == 0)
    def _():
        lend.wait_send()

    @pl.when(c == CORES - 1)
    def _():
        for y in vy_peers:
            remote(o3.at[y], in3.at[a], s3_r, i, y).wait_send()


def shards(tokens, var_embed, query, key_weight, value_weight, out_weight, var_slot):
    slots, batch, patches, width = tokens.shape
    nx, ny = lax.axis_size("vx"), lax.axis_size("vy")
    heads = HEADS
    patches = batch * patches
    rows, na, group, own = width // ny, ny // CORES, patches // nx, patches // (nx * ny)
    lane, lheads = width // CORES, heads // CORES
    chunks = len(pieces(lane)[0])
    held = CORES * slots * patches
    dma = pltpu.SemaphoreType.DMA
    vmem = pltpu.VMEM
    result = pl.pallas_call(
        functools.partial(kernel, nx, ny, heads),
        out_shape=vmem((own, width), BF16),
        in_specs=[pl.BlockSpec(memory_space=pl.ANY)] * 7,
        out_specs=pl.BlockSpec(memory_space=vmem),
        scratch_shapes=[
            vmem((CORES, slots, patches, width), BF16),
            vmem(var_embed.shape, BF16),
            vmem((width,), BF16),
            vmem((rows, width), BF16),
            vmem((CORES, rows, width), BF16),
            vmem((1, var_slot.shape[0]), jnp.int32),
            vmem((held, width), BF16),
            vmem((ny, rows, lane), BF16),
            vmem((rows, lane), BF16),
            vmem((CORES, 2, lheads, rows), BF16),
            vmem((ny, 2, lheads, rows), BF16),
            vmem((2 * lheads, width), BF16),
            vmem((held, lheads), BF16),
            vmem((nx, CORES, lheads, group), F32),
            vmem((nx * CORES, lheads, group), F32),
            vmem((CORES, lheads, group), F32),
            vmem((na, lheads, group), F32),
            vmem((nx, group, lane), F32),
            vmem((chunks, nx, group, lane // chunks), BF16),
            vmem((nx * CORES, group, lane // chunks), BF16),
            vmem((na // CORES, group, CORES * rows), BF16),
            vmem((na, group, CORES * rows), BF16),
            vmem((ny, own, width), BF16),
            vmem((na, own, width), BF16),
            vmem((held, lane), F32),
            vmem((held, lane), F32),
            vmem((patches, 128), F32),
            vmem((na, group, CORES * rows), F32),
            dma((10,)), dma, dma, dma((chunks, na)), dma((chunks, na)), dma, dma, dma, dma,
            dma, dma, dma,
        ],
        compiler_params=pltpu.CompilerParams(
            collective_id=0, has_side_effects=True, vmem_limit_bytes=56 * 1024 * 1024),
    )(
        tokens.reshape(slots, patches, width), var_embed, query,
        key_weight, value_weight, out_weight, var_slot.reshape(1, -1),
    )
    return result.reshape(batch, -1, width)


def solution(mesh):
    placed = (
        P(("vx", "vy"), None, None, None),
        P(),
        P(),
        P("vy", None),
        P("vy", None),
        P("vy", None),
        P(),
    )
    return jax.shard_map(
        shards, mesh=mesh, in_specs=placed, out_specs=P(None, ("vx", "vy"), None), check_vma=False
    )
```

```python
import functools
import math

import jax
import jax.numpy as jnp
from jax import lax
from jax.experimental import pallas as pl
from jax.experimental.pallas import tpu as pltpu
from jax.sharding import PartitionSpec as P

HEADS = 16
CORES = 2
LOWEST = -1e38
F32 = jnp.float32
BF16 = jnp.bfloat16
MESH = pl.DeviceIdType.MESH
NT = (((1,), (1,)), ((), ()))
TN = (((0,), (0,)), ((), ()))


def split(x):
    high = x.astype(BF16)
    return high, (x - high.astype(F32)).astype(BF16)


def dot(a, b):
    return jnp.dot(a, b, preferred_element_type=F32)


def pieces(lane):
    return (0, lane // 2), (lane // 2, lane // 2)


def flip(index, mask, size):
    bit = 1
    while bit < size:
        if mask & bit:
            index = index + bit - 2 * bit * (index // bit % 2)
        bit *= 2
    return index


def kernel(nx, ny, heads, tok_any, emb_any, qry_any, wk_any, wv_any, wo_any, slot_any, out,
           tok, emb, qry, wk, wo, slot, mixed, wbuf, wsrc, kq_mine, kq_in, kq_all, ex,
           stat, st_in, st2, st2_in, fexp, part, in1, p2, in2, o3, in3, early, spread_ex, tall, fz,
           load_s, send_s, kq_r, z_r, w_r, tok_r, wo_r, st_r, st2_r, s1_r, s2_r, s3_r):
    _, slots, patches, width = tok.shape
    rows = width // ny
    na = ny // CORES
    group = patches // nx
    piece = rows // nx
    lane = width // CORES
    starts, sizes = pieces(lane)
    chunks = len(starts)
    wide = CORES * rows
    first_plane = na // CORES
    own = patches // (nx * ny)
    hdim = width // heads
    lheads = heads // CORES
    cheads = lheads // CORES
    held_slots = CORES * slots
    block_rows = held_slots * group
    scale = 1.0 / math.sqrt(hdim)
    i = lax.axis_index("vx")
    j = lax.axis_index("vy")
    a = j // CORES
    c = j % CORES
    partner = a * CORES + (1 - c)
    x_peers = [flip(i, d, nx) for d in reversed(range(1, nx))]
    mirror = x_peers[0]
    a_peers = [flip(a, d, na) for d in range(1, na)]
    vy_peers = [lax.rem(j + d, ny) for d in range(1, ny)]

    def remote(src, dst, rs, x, y):
        return pltpu.make_async_remote_copy(
            src_ref=src, dst_ref=dst, send_sem=send_s, recv_sem=rs,
            device_id=(x, y), device_id_type=MESH)

    sent = []

    def send(*args):
        copy = remote(*args)
        copy.start()
        sent.append(copy)

    def arrived(ref, rs):
        remote(ref, ref, rs, i, j).wait_recv()

    barrier = pltpu.get_barrier_semaphore()
    for y in vy_peers:
        pl.semaphore_signal(barrier, inc=1, device_id=(i, y), device_id_type=MESH)
    for x in x_peers:
        pl.semaphore_signal(barrier, inc=1, device_id=(x, j), device_id_type=MESH)

    def cols(n):
        return slice(starts[n], starts[n] + sizes[n])

    def quarter(which, n):
        first = (which + CORES * (1 - n)) * sizes[n]
        if isinstance(which, int):
            return wv_any.at[:, first:first + sizes[n]]
        return wv_any.at[:, pl.ds(pl.multiple_of(first, sizes[n]), sizes[n])]

    pairs = ((wk_any, wk), (qry_any, qry),
             (quarter(0, 0), wsrc.at[0, :, cols(0)]), (quarter(1, 0), wsrc.at[1, :, cols(0)]),
             (quarter(0, 1), wsrc.at[0, :, cols(1)]), (quarter(1, 1), wsrc.at[1, :, cols(1)]),
             (quarter(c, 0), wbuf.at[j, :, cols(0)]), (quarter(c, 1), wbuf.at[j, :, cols(1)]),
             (tok_any, tok.at[c]), (emb_any, emb), (slot_any, slot), (wo_any, wo.at[c]))
    loads = [pltpu.make_async_copy(src, dst, load_s.at[n]) for n, (src, dst) in enumerate(pairs)]
    for load in loads:
        load.start()

    with jax.named_scope("A_load01"):
        loads[0].wait()
        loads[1].wait()
    head_row = lax.broadcasted_iota(jnp.int32, (heads, width), 0)
    head_col = lax.broadcasted_iota(jnp.int32, (heads, width), 1) // hdim
    qmat = jnp.where(head_row == head_col, jnp.broadcast_to(qry[...].astype(F32).reshape(1, width), (heads, width)), 0.0).astype(BF16)
    kq = lax.dot_general(qmat, wk[...], NT, preferred_element_type=F32)
    for d in range(CORES):
        for n in range(CORES):
            first = (d + CORES * (1 - n)) * cheads
            kq_high, kq_low = split(kq[first:first + cheads])
            kq_mine[d, 0, n * cheads:(n + 1) * cheads] = kq_high
            kq_mine[d, 1, n * cheads:(n + 1) * cheads] = kq_low

    with jax.named_scope("B_barrier"):
        pl.semaphore_wait(barrier, (ny - 1) + (nx - 1))


    def piece_rows(q):
        return pl.ds(pl.multiple_of(q * piece, piece), piece)

    with jax.named_scope("C_load23"):
        for load in loads[2:6]:
            load.wait()
    def along_z(q, n, x, sem):
        for d in range(CORES):
            send(wsrc.at[d, piece_rows(q), cols(n)], wbuf.at[j, piece_rows(q), cols(n)], sem, i, x * CORES + d)

    for n in range(chunks):
        for x in a_peers:
            along_z(i, n, x, z_r.at[n, a])
            if n == 0 and x is a_peers[0]:
                for y in vy_peers:
                    send(kq_mine.at[y % CORES], kq_in.at[j], kq_r, i, y)
        if n == 0:
            along_z(mirror, n, a_peers[0], w_r.at[n, a])
        send(wsrc.at[1 - c, :, cols(n)], wbuf.at[j, :, cols(n)], w_r.at[n, a], i, partner)
    with jax.named_scope("C_load4"):
        loads[8].wait()
    send(tok.at[c], tok.at[c], tok_r, i, partner)

    kq_in[j] = kq_mine[c]

    def pair_rows(x, q, n):
        return wbuf.at[pl.ds(pl.multiple_of(x * CORES, CORES), CORES), piece_rows(q), cols(n)]

    def share(n, x):
        here = pair_rows(x, i, n)
        arrived(here, z_r.at[n, x])
        for q in x_peers[1:] if n > 0 or x is a_peers[0] else x_peers:
            send(here, here, w_r.at[n, x], q, j)

    def complete(n, sources):
        for x in sources:
            if x is a:
                arrived(wbuf.at[partner, :, cols(n)], w_r.at[n, a])
            else:
                arrived(wbuf.at[pl.ds(pl.multiple_of(x * CORES, CORES), CORES), 0:(nx - 1) * piece, cols(n)], w_r.at[n, x])

    with jax.named_scope("D_loads"):
        for load in loads[6:8] + loads[9:]:
            load.wait()
    count = slot.shape[1]
    padded = -(-held_slots // 8) * 8
    ids = (i * ny + a * CORES) * slots + lax.broadcasted_iota(jnp.int32, (padded, count), 0)
    match = jnp.where(ids == jnp.broadcast_to(slot[...], (padded, count)), 1.0, 0.0)
    held = jnp.max(match, axis=1, keepdims=True)
    embed = dot(match.astype(BF16), emb[...])

    def mix(core):
        for s in range(slots):
            m = core * slots + s
            line = jnp.sum(jnp.where(lax.broadcasted_iota(jnp.int32, (padded, width), 0) == m, embed, 0.0), axis=0, keepdims=True)
            for g in range(nx):
                first = pl.multiple_of(g * block_rows + m * group, group)
                mixed[pl.ds(first, group), :] = (tok[core, s, g * group:(g + 1) * group, :].astype(F32) + line).astype(BF16)

    lend = remote(wo.at[0], wo.at[0], wo_r, i, partner)

    @pl.when(c == 0)
    def _():
        lend.start()

    with jax.named_scope("E_mix"):
        mix(c)
    with jax.named_scope("F_share00"):
        share(0, a_peers[0])
    with jax.named_scope("G_tok"):
        arrived(tok.at[1 - c], tok_r)
    with jax.named_scope("G_mix2"):
        mix(1 - c)
    with jax.named_scope("G_share01"):
        for x in a_peers[1:-1]:
            share(0, x)
    for n in range(1, chunks):
        for x in a_peers:
            along_z(mirror, n, x, w_r.at[n, a])
    with jax.named_scope("J_share02"):
        share(0, a_peers[-1])
    with jax.named_scope("H_kq"):
        arrived(kq_in.at[0:ny - 1], kq_r)
    for y in range(ny):
        for d in range(2):
            kq_all[d * lheads:(d + 1) * lheads, y * rows:(y + 1) * rows] = kq_in[y, d]
    for g in range(nx):
        both = lax.dot_general(mixed[g * block_rows:(g + 1) * block_rows, :], kq_all[...], NT, preferred_element_type=F32)
        score = scale * (both[:, 0:lheads] + both[:, lheads:2 * lheads])
        top = jnp.full((group, lheads), LOWEST, F32)
        scores = []
        for s in range(held_slots):
            here = jnp.where(held[s:s + 1, :] > 0, score[s * group:(s + 1) * group], LOWEST)
            scores.append(here)
            top = jnp.maximum(top, here)
        total = jnp.zeros((group, lheads), F32)
        for s in range(held_slots):
            e = jnp.where(held[s:s + 1, :] > 0, jnp.exp(scores[s] - top), 0.0).astype(BF16)
            ex[g * block_rows + s * group:g * block_rows + (s + 1) * group, :] = e
            total += e.astype(F32)
        tall[g * group:(g + 1) * group, 0:lheads] = top
        tall[g * group:(g + 1) * group, lheads:2 * lheads] = total
    flat = tall[...].T
    for g in range(nx):
        stat[g] = flat[0:2 * lheads, g * group:(g + 1) * group]

    def lend_stats():
        return remote(stat.at[i], st_in.at[i * CORES], st_r, i, partner)

    for q in x_peers:
        send(stat.at[q], st_in.at[i * CORES + c], st_r, q, a * CORES + CORES - 1)

    @pl.when(c == 0)
    def _():
        lend_stats().start()

    @pl.when(c == CORES - 1)
    def _():
        st_in[i * CORES + c] = stat[i]

    with jax.named_scope("J_share1"):
        for n in range(1, chunks):
            for x in a_peers:
                share(n, x)

    def group_rows(g):
        return slice(g * block_rows, (g + 1) * block_rows)

    feature = lax.broadcasted_iota(jnp.int32, (lheads, lane), 1)
    spread = jnp.where(feature // hdim == lax.broadcasted_iota(jnp.int32, (lheads, lane), 0), 1.0, 0.0).astype(BF16)

    def plane_product(x, here, where):
        first = pl.multiple_of(x * wide, wide)
        weight = wbuf[pl.ds(pl.multiple_of(x * CORES, CORES), CORES), :, where].reshape(wide, -1)
        return dot(mixed[here, pl.ds(first, wide)], weight)

    def project_early(n, sources, more=False):
        for g in range(nx):
            here = group_rows(g)
            value = sum(plane_product(x, here, cols(n)) for x in sources)
            early[here, cols(n)] = value + early[here, cols(n)] if more else value

    def give(n, g):
        return remote(part.at[n, g], in1.at[n, i * CORES + c], s1_r.at[n], g, a * CORES + CORES - 1)

    def project_late(n, sources):
        for batch in (range(2), range(2, nx)):
            for g in batch:
                here = group_rows(g)
                value = sum(plane_product(x, here, cols(n)) for x in sources)
                value = (value + early[here, cols(n)]) * spread_ex[here, cols(n)]
                part[n, g] = sum(value[s * group:(s + 1) * group] for s in range(held_slots)).astype(BF16)
            for g in batch:
                @pl.when(i != g)
                def _():
                    give(n, g).start()

        for q in x_peers:
            sent.append(give(n, q))

        @pl.when(c == CORES - 1)
        def _():
            in1[n, i * CORES + c] = part[n, i]

        @pl.when(c == 0)
        def _():
            give(n, i).start()

    half_planes = first_plane // CORES
    targets = [(d, k) for d in reversed(range(CORES)) for k in range(half_planes)]

    def target_of(d, k, n):
        return ((d + CORES * (1 - n)) * half_planes + k) * CORES + CORES - 1

    def scatter(d, k, n):
        return remote(p2.at[n, d * half_planes + k], in2.at[a], s2_r, i, target_of(d, k, n))

    def scatter_stats(d, k, n):
        return remote(st2.at[d, n], st2_in.at[a], st2_r, i, target_of(d, k, n))

    def plane_stats():
        with jax.named_scope("K_st"):
            arrived(st_in.at[0:nx * CORES - 1], st_r)
        for d in range(CORES):
            tops = [st_in[q * CORES + d, 0:lheads] for q in range(nx)]
            high = functools.reduce(jnp.maximum, tops)
            below = [jnp.exp(top - high) for top in tops]
            total = sum(below[q] * st_in[q * CORES + d, lheads:2 * lheads] for q in range(nx))
            for n in range(chunks):
                heads_n = slice(n * cheads, (n + 1) * cheads)
                st2[d, n, 0:cheads] = high[heads_n]
                st2[d, n, cheads:lheads] = total[heads_n]
            for q in range(nx):
                f_high, f_low = split(below[q])
                fexp[q * CORES + d] = (lax.dot_general(f_high, spread, TN, preferred_element_type=F32)
                                       + lax.dot_general(f_low, spread, TN, preferred_element_type=F32))
        for n in range(chunks):
            for d, k in targets:
                @pl.when(target_of(d, k, n) != j)
                def _():
                    scatter_stats(d, k, n).start()

    def combine(n):
        arrived(in1.at[n, 0:nx * CORES - 1], s1_r.at[n])
        for d in reversed(range(CORES)):
            acc = sum(fexp[q * CORES + d, :, cols(n)] * in1[n, q * CORES + d].astype(F32) for q in range(nx))
            for k in range(half_planes):
                p2[n, d * half_planes + k] = acc[:, k * wide:(k + 1) * wide].astype(BF16)

                @pl.when(target_of(d, k, n) != j)
                def _():
                    scatter(d, k, n).start()

    spread_ex[...] = dot(ex[...], spread)
    with jax.named_scope("K_complete0"):
        complete(0, [a] + a_peers[:-2])
    with jax.named_scope("K_early0"):
        project_early(0, [a] + a_peers[:-2])
    with jax.named_scope("L_complete0"):
        complete(0, a_peers[-2:])
    with jax.named_scope("M_project0"):
        project_late(0, a_peers[-2:])
    @pl.when(c == CORES - 1)
    def _():
        plane_stats()

    for n in range(1, chunks):
        with jax.named_scope("O_early1"):
            complete(n, [a])
            project_early(n, [a])
        with jax.named_scope("O_complete1"):
            complete(n, a_peers[:-1])
        with jax.named_scope("O_early2"):
            project_early(n, a_peers[:-1], True)
        with jax.named_scope("O_complete2"):
            complete(n, a_peers[-1:])
        with jax.named_scope("P_project1"):
            project_late(n, a_peers[-1:])
    block = a // half_planes
    spot = lax.rem(a, half_planes)
    my_chunk = 1 - block // CORES
    my_lane = lax.rem(block, CORES)
    side = a // first_plane
    fold = a + side * (na - 1 - 2 * a)
    steps = [na - 1 - k - (k + fold + 1) // na for k in range(na - 1)]
    far_first = [p + side * (na - 1 - 2 * p) for p in steps]
    turned = (1 - side) * ((a + na - 1) // na)
    root_first = [far_first[k] + turned * (far_first[k - 1] - far_first[k]) for k in range(na - 1)]

    @pl.when(c == CORES - 1)
    def _():
        for n in range(chunks):
            with jax.named_scope(f"R_combine{n}"):
                combine(n)
        st2_in[a] = st2[my_lane, my_chunk]
        in2[a] = p2[my_chunk, my_lane * half_planes + spot]
        arrived(st2_in.at[0:na - 1], st2_r)

        highest = functools.reduce(jnp.maximum, [st2_in[p, 0:cheads] for p in range(na)])
        lower = [jnp.exp(st2_in[p, 0:cheads] - highest) for p in range(na)]
        whole = sum(lower[p] * st2_in[p, cheads:lheads] for p in range(na))
        wanted = (spot * wide + lax.broadcasted_iota(jnp.int32, (cheads, wide), 1)) // hdim
        widen = jnp.where(wanted == lax.broadcasted_iota(jnp.int32, (cheads, wide), 0), 1.0, 0.0).astype(BF16)
        for p in range(na):
            f_high, f_low = split(lower[p] / whole)
            fz[p] = (lax.dot_general(f_high, widen, TN, preferred_element_type=F32)
                     + lax.dot_general(f_low, widen, TN, preferred_element_type=F32))
        arrived(wo.at[0], wo_r)

        with jax.named_scope("S_in2"):
            arrived(in2.at[0:na - 1], s2_r)

        acc = sum(fz[p] * in2[p].astype(F32) for p in range(na))
        result = dot(acc.astype(BF16), wo[...].reshape(wide, width)).astype(BF16)
        for y in range(ny):
            o3[y] = result[y * own:(y + 1) * own]
        for x in root_first:
            for d in range(CORES):
                remote(o3.at[x * CORES + d], in3.at[a], s3_r, i, x * CORES + d).start()
        remote(o3.at[partner], in3.at[a], s3_r, i, partner).start()
        in3[a] = o3[j]
        with jax.named_scope("T_in3n"):
            arrived(in3.at[0:na - 1], s3_r)

    @pl.when(c != CORES - 1)
    def _():
        with jax.named_scope("T_in3s"):
            arrived(in3, s3_r)

    final = sum(in3[x].astype(F32) for x in range(na))
    out[...] = final.astype(BF16)
    with jax.named_scope("U_sends"):
        for copy in sent:
            copy.wait_send()
    @pl.when(c == 0)
    def _():
        lend.wait_send()
        lend_stats().wait_send()
        for n in range(chunks):
            give(n, i).wait_send()

    @pl.when(c == CORES - 1)
    def _():
        for n in range(chunks):
            for d, k in targets:
                @pl.when(target_of(d, k, n) != j)
                def _():
                    scatter(d, k, n).wait_send()
                    scatter_stats(d, k, n).wait_send()
        for y in vy_peers:
            remote(o3.at[y], in3.at[a], s3_r, i, y).wait_send()


def shards(tokens, var_embed, query, key_weight, value_weight, out_weight, var_slot):
    slots, batch, patches, width = tokens.shape
    nx, ny = lax.axis_size("vx"), lax.axis_size("vy")
    heads = HEADS
    patches = batch * patches
    rows, na, group, own = width // ny, ny // CORES, patches // nx, patches // (nx * ny)
    lane, lheads = width // CORES, heads // CORES
    chunks = len(pieces(lane)[0])
    held = CORES * slots * patches
    dma = pltpu.SemaphoreType.DMA
    vmem = pltpu.VMEM
    result = pl.pallas_call(
        functools.partial(kernel, nx, ny, heads),
        out_shape=vmem((own, width), BF16),
        in_specs=[pl.BlockSpec(memory_space=pl.ANY)] * 7,
        out_specs=pl.BlockSpec(memory_space=vmem),
        scratch_shapes=[
            vmem((CORES, slots, patches, width), BF16),
            vmem(var_embed.shape, BF16),
            vmem((width,), BF16),
            vmem((rows, width), BF16),
            vmem((CORES, rows, width), BF16),
            vmem((1, var_slot.shape[0]), jnp.int32),
            vmem((held, width), BF16),
            vmem((ny, rows, lane), BF16),
            vmem((CORES, rows, lane), BF16),
            vmem((CORES, 2, lheads, rows), BF16),
            vmem((ny, 2, lheads, rows), BF16),
            vmem((2 * lheads, width), BF16),
            vmem((held, lheads), BF16),
            vmem((nx, 2 * lheads, group), F32),
            vmem((nx * CORES, 2 * lheads, group), F32),
            vmem((CORES, chunks, lheads, group), F32),
            vmem((na, lheads, group), F32),
            vmem((nx * CORES, group, lane), F32),
            vmem((chunks, nx, group, lane // chunks), BF16),
            vmem((chunks, nx * CORES, group, lane // chunks), BF16),
            vmem((chunks, na // CORES, group, CORES * rows), BF16),
            vmem((na, group, CORES * rows), BF16),
            vmem((ny, own, width), BF16),
            vmem((na, own, width), BF16),
            vmem((held, lane), F32),
            vmem((held, lane), F32),
            vmem((patches, 128), F32),
            vmem((na, group, CORES * rows), F32),
            dma((12,)), dma, dma, dma((chunks, na)), dma((chunks, na)), dma, dma, dma, dma,
            dma((chunks,)), dma, dma,
        ],
        compiler_params=pltpu.CompilerParams(
            collective_id=0, has_side_effects=True, vmem_limit_bytes=56 * 1024 * 1024),
    )(
        tokens.reshape(slots, patches, width), var_embed, query,
        key_weight, value_weight, out_weight, var_slot.reshape(1, -1),
    )
    return result.reshape(batch, -1, width)


def solution(mesh):
    placed = (
        P(("vx", "vy"), None, None, None),
        P(),
        P(),
        P("vy", None),
        P("vy", None),
        P("vy", None),
        P(),
    )
    return jax.shard_map(
        shards, mesh=mesh, in_specs=placed, out_specs=P(None, ("vx", "vy"), None), check_vma=False
    )
```

```python
import functools
import math

import jax
import jax.numpy as jnp
from jax import lax
from jax.experimental import pallas as pl
from jax.experimental.pallas import tpu as pltpu
from jax.sharding import PartitionSpec as P

HEADS = 16
CORES = 2
LOWEST = -1e38
F32 = jnp.float32
BF16 = jnp.bfloat16
MESH = pl.DeviceIdType.MESH
NT = (((1,), (1,)), ((), ()))
TN = (((0,), (0,)), ((), ()))


def split(x):
    high = x.astype(BF16)
    return high, (x - high.astype(F32)).astype(BF16)


def dot(a, b):
    return jnp.dot(a, b, preferred_element_type=F32)


def pieces(lane):
    return (0, lane // 2), (lane // 2, lane // 2)


def flip(index, mask, size):
    bit = 1
    while bit < size:
        if mask & bit:
            index = index + bit - 2 * bit * (index // bit % 2)
        bit *= 2
    return index


def kernel(nx, ny, heads, tok_any, emb_any, qry_any, wk_any, wv_any, wo_any, slot_any, out,
           tok, emb, qry, wk, wo, slot, mixed, wbuf, wsrc, kq_mine, kq_in, kq_all, ex,
           stat, st_in, st2, st2_in, fexp, part, in1, p2, in2, o3, in3, early, spread_ex, tall, fz,
           load_s, send_s, kq_r, z_r, w_r, tok_r, wo_r, st_r, st2_r, s1_r, s2_r, s3_r):
    _, slots, patches, width = tok.shape
    rows = width // ny
    na = ny // CORES
    group = patches // nx
    piece = rows // nx
    lane = width // CORES
    starts, sizes = pieces(lane)
    chunks = len(starts)
    wide = CORES * rows
    first_plane = na // CORES
    own = patches // (nx * ny)
    hdim = width // heads
    lheads = heads // CORES
    cheads = lheads // CORES
    held_slots = CORES * slots
    block_rows = held_slots * group
    scale = 1.0 / math.sqrt(hdim)
    i = lax.axis_index("vx")
    j = lax.axis_index("vy")
    a = j // CORES
    c = j % CORES
    partner = a * CORES + (1 - c)
    x_peers = [flip(i, d, nx) for d in reversed(range(1, nx))]
    mirror = x_peers[0]
    a_peers = [flip(a, d, na) for d in range(1, na)]
    vy_peers = [lax.rem(j + d, ny) for d in range(1, ny)]

    def remote(src, dst, rs, x, y):
        return pltpu.make_async_remote_copy(
            src_ref=src, dst_ref=dst, send_sem=send_s, recv_sem=rs,
            device_id=(x, y), device_id_type=MESH)

    sent = []

    def send(*args):
        copy = remote(*args)
        copy.start()
        sent.append(copy)

    def arrived(ref, rs):
        remote(ref, ref, rs, i, j).wait_recv()

    barrier = pltpu.get_barrier_semaphore()
    for y in vy_peers:
        pl.semaphore_signal(barrier, inc=1, device_id=(i, y), device_id_type=MESH)
    for x in x_peers:
        pl.semaphore_signal(barrier, inc=1, device_id=(x, j), device_id_type=MESH)

    def cols(n):
        return slice(starts[n], starts[n] + sizes[n])

    def quarter(which, n):
        first = (which + CORES * (1 - n)) * sizes[n]
        if isinstance(which, int):
            return wv_any.at[:, first:first + sizes[n]]
        return wv_any.at[:, pl.ds(pl.multiple_of(first, sizes[n]), sizes[n])]

    pairs = ((wk_any, wk), (qry_any, qry),
             (quarter(0, 0), wsrc.at[0, :, cols(0)]), (quarter(1, 0), wsrc.at[1, :, cols(0)]),
             (quarter(0, 1), wsrc.at[0, :, cols(1)]), (quarter(1, 1), wsrc.at[1, :, cols(1)]),
             (quarter(c, 0), wbuf.at[j, :, cols(0)]), (quarter(c, 1), wbuf.at[j, :, cols(1)]),
             (tok_any, tok.at[c]), (emb_any, emb), (slot_any, slot), (wo_any, wo.at[c]))
    loads = [pltpu.make_async_copy(src, dst, load_s.at[n]) for n, (src, dst) in enumerate(pairs)]
    for load in loads:
        load.start()

    with jax.named_scope("A_load01"):
        loads[0].wait()
        loads[1].wait()
    head_row = lax.broadcasted_iota(jnp.int32, (heads, width), 0)
    head_col = lax.broadcasted_iota(jnp.int32, (heads, width), 1) // hdim
    qmat = jnp.where(head_row == head_col, jnp.broadcast_to(qry[...].astype(F32).reshape(1, width), (heads, width)), 0.0).astype(BF16)
    kq = lax.dot_general(qmat, wk[...], NT, preferred_element_type=F32)
    for d in range(CORES):
        for n in range(CORES):
            first = (d + CORES * (1 - n)) * cheads
            kq_high, kq_low = split(kq[first:first + cheads])
            kq_mine[d, 0, n * cheads:(n + 1) * cheads] = kq_high
            kq_mine[d, 1, n * cheads:(n + 1) * cheads] = kq_low

    with jax.named_scope("B_barrier"):
        pl.semaphore_wait(barrier, (ny - 1) + (nx - 1))


    def piece_rows(q):
        return pl.ds(pl.multiple_of(q * piece, piece), piece)

    with jax.named_scope("C_load23"):
        for load in loads[2:6]:
            load.wait()
    def along_z(q, n, x, sem):
        for d in range(CORES):
            send(wsrc.at[d, piece_rows(q), cols(n)], wbuf.at[j, piece_rows(q), cols(n)], sem, i, x * CORES + d)

    for n in range(chunks):
        for x in a_peers:
            along_z(i, n, x, z_r.at[n, a])
            if n == 0 and x is a_peers[0]:
                for y in vy_peers:
                    send(kq_mine.at[y % CORES], kq_in.at[j], kq_r, i, y)
        if n == 0:
            along_z(mirror, n, a_peers[0], w_r.at[n, a])
        send(wsrc.at[1 - c, :, cols(n)], wbuf.at[j, :, cols(n)], w_r.at[n, a], i, partner)
    with jax.named_scope("C_load4"):
        loads[8].wait()
    send(tok.at[c], tok.at[c], tok_r, i, partner)

    kq_in[j] = kq_mine[c]

    def pair_rows(x, q, n):
        return wbuf.at[pl.ds(pl.multiple_of(x * CORES, CORES), CORES), piece_rows(q), cols(n)]

    def share(n, x):
        here = pair_rows(x, i, n)
        arrived(here, z_r.at[n, x])
        for q in x_peers[1:] if n > 0 or x is a_peers[0] else x_peers:
            send(here, here, w_r.at[n, x], q, j)

    def complete(n, sources):
        for x in sources:
            if x is a:
                arrived(wbuf.at[partner, :, cols(n)], w_r.at[n, a])
            else:
                arrived(wbuf.at[pl.ds(pl.multiple_of(x * CORES, CORES), CORES), 0:(nx - 1) * piece, cols(n)], w_r.at[n, x])

    with jax.named_scope("D_loads"):
        for load in loads[6:8] + loads[9:]:
            load.wait()
    count = slot.shape[1]
    padded = -(-held_slots // 8) * 8
    ids = (i * ny + a * CORES) * slots + lax.broadcasted_iota(jnp.int32, (padded, count), 0)
    match = jnp.where(ids == jnp.broadcast_to(slot[...], (padded, count)), 1.0, 0.0)
    held = jnp.max(match, axis=1, keepdims=True)
    embed = dot(match.astype(BF16), emb[...])

    def mix(core):
        for s in range(slots):
            m = core * slots + s
            line = jnp.sum(jnp.where(lax.broadcasted_iota(jnp.int32, (padded, width), 0) == m, embed, 0.0), axis=0, keepdims=True)
            for g in range(nx):
                first = pl.multiple_of(g * block_rows + m * group, group)
                mixed[pl.ds(first, group), :] = (tok[core, s, g * group:(g + 1) * group, :].astype(F32) + line).astype(BF16)

    lend = remote(wo.at[0], wo.at[0], wo_r, i, partner)

    @pl.when(c == 0)
    def _():
        lend.start()

    with jax.named_scope("E_mix"):
        mix(c)
    with jax.named_scope("F_share00"):
        share(0, a_peers[0])
    with jax.named_scope("G_tok"):
        arrived(tok.at[1 - c], tok_r)
    with jax.named_scope("G_mix2"):
        mix(1 - c)
    with jax.named_scope("G_share01"):
        for x in a_peers[1:-1]:
            share(0, x)
    for n in range(1, chunks):
        for x in a_peers:
            along_z(mirror, n, x, w_r.at[n, a])
    with jax.named_scope("J_share02"):
        share(0, a_peers[-1])
    with jax.named_scope("H_kq"):
        arrived(kq_in.at[0:ny - 1], kq_r)
    for y in range(ny):
        for d in range(2):
            kq_all[d * lheads:(d + 1) * lheads, y * rows:(y + 1) * rows] = kq_in[y, d]
    for g in range(nx):
        both = lax.dot_general(mixed[g * block_rows:(g + 1) * block_rows, :], kq_all[...], NT, preferred_element_type=F32)
        score = scale * (both[:, 0:lheads] + both[:, lheads:2 * lheads])
        top = jnp.full((group, lheads), LOWEST, F32)
        scores = []
        for s in range(held_slots):
            here = jnp.where(held[s:s + 1, :] > 0, score[s * group:(s + 1) * group], LOWEST)
            scores.append(here)
            top = jnp.maximum(top, here)
        total = jnp.zeros((group, lheads), F32)
        for s in range(held_slots):
            e = jnp.where(held[s:s + 1, :] > 0, jnp.exp(scores[s] - top), 0.0).astype(BF16)
            ex[g * block_rows + s * group:g * block_rows + (s + 1) * group, :] = e
            total += e.astype(F32)
        tall[g * group:(g + 1) * group, 0:lheads] = top
        tall[g * group:(g + 1) * group, lheads:2 * lheads] = total
    flat = tall[...].T
    for g in range(nx):
        stat[g] = flat[0:2 * lheads, g * group:(g + 1) * group]

    def lend_stats():
        return remote(stat.at[i], st_in.at[i * CORES], st_r, i, partner)

    for q in x_peers:
        send(stat.at[q], st_in.at[i * CORES + c], st_r, q, a * CORES + CORES - 1)

    @pl.when(c == 0)
    def _():
        lend_stats().start()

    @pl.when(c == CORES - 1)
    def _():
        st_in[i * CORES + c] = stat[i]

    with jax.named_scope("J_share1"):
        for n in range(1, chunks):
            for x in a_peers:
                share(n, x)

    def group_rows(g):
        return slice(g * block_rows, (g + 1) * block_rows)

    feature = lax.broadcasted_iota(jnp.int32, (lheads, lane), 1)
    spread = jnp.where(feature // hdim == lax.broadcasted_iota(jnp.int32, (lheads, lane), 0), 1.0, 0.0).astype(BF16)

    def plane_product(x, here, where):
        first = pl.multiple_of(x * wide, wide)
        weight = wbuf[pl.ds(pl.multiple_of(x * CORES, CORES), CORES), :, where].reshape(wide, -1)
        return dot(mixed[here, pl.ds(first, wide)], weight)

    def project_early(n, sources, more=False):
        for g in range(nx):
            here = group_rows(g)
            value = sum(plane_product(x, here, cols(n)) for x in sources)
            early[here, cols(n)] = value + early[here, cols(n)] if more else value

    def give(n, g):
        return remote(part.at[n, g], in1.at[n, i * CORES + c], s1_r.at[n], g, a * CORES + CORES - 1)

    def project_late(n, sources):
        for batch in (range(2), range(2, nx)):
            for g in batch:
                here = group_rows(g)
                value = sum(plane_product(x, here, cols(n)) for x in sources)
                value = (value + early[here, cols(n)]) * spread_ex[here, cols(n)]
                part[n, g] = sum(value[s * group:(s + 1) * group] for s in range(held_slots)).astype(BF16)
            for g in batch:
                @pl.when(i != g)
                def _():
                    give(n, g).start()

        for q in x_peers:
            sent.append(give(n, q))

        @pl.when(c == CORES - 1)
        def _():
            in1[n, i * CORES + c] = part[n, i]

        @pl.when(c == 0)
        def _():
            give(n, i).start()

    half_planes = first_plane // CORES
    targets = [(d, k) for d in reversed(range(CORES)) for k in range(half_planes)]

    def target_of(d, k, n):
        return ((d + CORES * (1 - n)) * half_planes + k) * CORES + CORES - 1

    def scatter(d, k, n):
        return remote(p2.at[n, d * half_planes + k], in2.at[a], s2_r, i, target_of(d, k, n))

    def scatter_stats(d, k, n):
        return remote(st2.at[d, n], st2_in.at[a], st2_r, i, target_of(d, k, n))

    def plane_stats():
        with jax.named_scope("K_st"):
            arrived(st_in.at[0:nx * CORES - 1], st_r)
        for d in range(CORES):
            tops = [st_in[q * CORES + d, 0:lheads] for q in range(nx)]
            high = functools.reduce(jnp.maximum, tops)
            below = [jnp.exp(top - high) for top in tops]
            total = sum(below[q] * st_in[q * CORES + d, lheads:2 * lheads] for q in range(nx))
            for n in range(chunks):
                heads_n = slice(n * cheads, (n + 1) * cheads)
                st2[d, n, 0:cheads] = high[heads_n]
                st2[d, n, cheads:lheads] = total[heads_n]
            for q in range(nx):
                f_high, f_low = split(below[q])
                fexp[q * CORES + d] = (lax.dot_general(f_high, spread, TN, preferred_element_type=F32)
                                       + lax.dot_general(f_low, spread, TN, preferred_element_type=F32))
        for n in range(chunks):
            for d, k in targets:
                @pl.when(target_of(d, k, n) != j)
                def _():
                    scatter_stats(d, k, n).start()

    def combine(n):
        arrived(in1.at[n, 0:nx * CORES - 1], s1_r.at[n])
        for d in reversed(range(CORES)):
            acc = sum(fexp[q * CORES + d, :, cols(n)] * in1[n, q * CORES + d].astype(F32) for q in range(nx))
            for k in range(half_planes):
                p2[n, d * half_planes + k] = acc[:, k * wide:(k + 1) * wide].astype(BF16)

                @pl.when(target_of(d, k, n) != j)
                def _():
                    scatter(d, k, n).start()

    spread_ex[...] = dot(ex[...], spread)
    with jax.named_scope("K_complete0"):
        complete(0, [a] + a_peers[:-2])
    with jax.named_scope("K_early0"):
        project_early(0, [a] + a_peers[:-2])
    with jax.named_scope("L_complete0"):
        complete(0, a_peers[-2:])
    with jax.named_scope("M_project0"):
        project_late(0, a_peers[-2:])
    @pl.when(c == CORES - 1)
    def _():
        plane_stats()

    for n in range(1, chunks):
        with jax.named_scope("O_early1"):
            complete(n, [a])
            project_early(n, [a])
        with jax.named_scope("O_complete1"):
            complete(n, a_peers[:-1])
        with jax.named_scope("O_early2"):
            project_early(n, a_peers[:-1], True)
        with jax.named_scope("O_complete2"):
            complete(n, a_peers[-1:])
        with jax.named_scope("P_project1"):
            project_late(n, a_peers[-1:])
    block = a // half_planes
    spot = lax.rem(a, half_planes)
    my_chunk = 1 - block // CORES
    my_lane = lax.rem(block, CORES)
    root_first = [k + (k + na - a) // na for k in range(na - 1)]

    @pl.when(c == CORES - 1)
    def _():
        for n in range(chunks):
            with jax.named_scope(f"R_combine{n}"):
                combine(n)
        st2_in[a] = st2[my_lane, my_chunk]
        in2[a] = p2[my_chunk, my_lane * half_planes + spot]
        arrived(st2_in.at[0:na - 1], st2_r)

        highest = functools.reduce(jnp.maximum, [st2_in[p, 0:cheads] for p in range(na)])
        lower = [jnp.exp(st2_in[p, 0:cheads] - highest) for p in range(na)]
        whole = sum(lower[p] * st2_in[p, cheads:lheads] for p in range(na))
        wanted = (spot * wide + lax.broadcasted_iota(jnp.int32, (cheads, wide), 1)) // hdim
        widen = jnp.where(wanted == lax.broadcasted_iota(jnp.int32, (cheads, wide), 0), 1.0, 0.0).astype(BF16)
        for p in range(na):
            f_high, f_low = split(lower[p] / whole)
            fz[p] = (lax.dot_general(f_high, widen, TN, preferred_element_type=F32)
                     + lax.dot_general(f_low, widen, TN, preferred_element_type=F32))
        arrived(wo.at[0], wo_r)

        with jax.named_scope("S_in2"):
            arrived(in2.at[0:na - 1], s2_r)

        acc = sum(fz[p] * in2[p].astype(F32) for p in range(na))
        result = dot(acc.astype(BF16), wo[...].reshape(wide, width)).astype(BF16)
        for y in range(ny):
            o3[y] = result[y * own:(y + 1) * own]
        for x in root_first:
            for d in range(CORES):
                remote(o3.at[x * CORES + d], in3.at[a], s3_r, i, x * CORES + d).start()
        remote(o3.at[partner], in3.at[a], s3_r, i, partner).start()
        in3[a] = o3[j]
        with jax.named_scope("T_in3n"):
            arrived(in3.at[0:na - 1], s3_r)

    @pl.when(c != CORES - 1)
    def _():
        with jax.named_scope("T_in3s"):
            arrived(in3, s3_r)

    final = sum(in3[x].astype(F32) for x in range(na))
    out[...] = final.astype(BF16)
    with jax.named_scope("U_sends"):
        for copy in sent:
            copy.wait_send()
    @pl.when(c == 0)
    def _():
        lend.wait_send()
        lend_stats().wait_send()
        for n in range(chunks):
            give(n, i).wait_send()

    @pl.when(c == CORES - 1)
    def _():
        for n in range(chunks):
            for d, k in targets:
                @pl.when(target_of(d, k, n) != j)
                def _():
                    scatter(d, k, n).wait_send()
                    scatter_stats(d, k, n).wait_send()
        for y in vy_peers:
            remote(o3.at[y], in3.at[a], s3_r, i, y).wait_send()


def shards(tokens, var_embed, query, key_weight, value_weight, out_weight, var_slot):
    slots, batch, patches, width = tokens.shape
    nx, ny = lax.axis_size("vx"), lax.axis_size("vy")
    heads = HEADS
    patches = batch * patches
    rows, na, group, own = width // ny, ny // CORES, patches // nx, patches // (nx * ny)
    lane, lheads = width // CORES, heads // CORES
    chunks = len(pieces(lane)[0])
    held = CORES * slots * patches
    dma = pltpu.SemaphoreType.DMA
    vmem = pltpu.VMEM
    result = pl.pallas_call(
        functools.partial(kernel, nx, ny, heads),
        out_shape=vmem((own, width), BF16),
        in_specs=[pl.BlockSpec(memory_space=pl.ANY)] * 7,
        out_specs=pl.BlockSpec(memory_space=vmem),
        scratch_shapes=[
            vmem((CORES, slots, patches, width), BF16),
            vmem(var_embed.shape, BF16),
            vmem((width,), BF16),
            vmem((rows, width), BF16),
            vmem((CORES, rows, width), BF16),
            vmem((1, var_slot.shape[0]), jnp.int32),
            vmem((held, width), BF16),
            vmem((ny, rows, lane), BF16),
            vmem((CORES, rows, lane), BF16),
            vmem((CORES, 2, lheads, rows), BF16),
            vmem((ny, 2, lheads, rows), BF16),
            vmem((2 * lheads, width), BF16),
            vmem((held, lheads), BF16),
            vmem((nx, 2 * lheads, group), F32),
            vmem((nx * CORES, 2 * lheads, group), F32),
            vmem((CORES, chunks, lheads, group), F32),
            vmem((na, lheads, group), F32),
            vmem((nx * CORES, group, lane), F32),
            vmem((chunks, nx, group, lane // chunks), BF16),
            vmem((chunks, nx * CORES, group, lane // chunks), BF16),
            vmem((chunks, na // CORES, group, CORES * rows), BF16),
            vmem((na, group, CORES * rows), BF16),
            vmem((ny, own, width), BF16),
            vmem((na, own, width), BF16),
            vmem((held, lane), F32),
            vmem((held, lane), F32),
            vmem((patches, 128), F32),
            vmem((na, group, CORES * rows), F32),
            dma((12,)), dma, dma, dma((chunks, na)), dma((chunks, na)), dma, dma, dma, dma,
            dma((chunks,)), dma, dma,
        ],
        compiler_params=pltpu.CompilerParams(
            collective_id=0, has_side_effects=True, vmem_limit_bytes=56 * 1024 * 1024),
    )(
        tokens.reshape(slots, patches, width), var_embed, query,
        key_weight, value_weight, out_weight, var_slot.reshape(1, -1),
    )
    return result.reshape(batch, -1, width)


def solution(mesh):
    placed = (
        P(("vx", "vy"), None, None, None),
        P(),
        P(),
        P("vy", None),
        P("vy", None),
        P("vy", None),
        P(),
    )
    return jax.shard_map(
        shards, mesh=mesh, in_specs=placed, out_specs=P(None, ("vx", "vy"), None), check_vma=False
    )
```

```python
import functools
import math

import jax
import jax.numpy as jnp
from jax import lax
from jax.experimental import pallas as pl
from jax.experimental.pallas import tpu as pltpu
from jax.sharding import PartitionSpec as P

HEADS = 16
CORES = 2
LOWEST = -1e38
F32 = jnp.float32
BF16 = jnp.bfloat16
MESH = pl.DeviceIdType.MESH
NT = (((1,), (1,)), ((), ()))
TN = (((0,), (0,)), ((), ()))


def split(x):
    high = x.astype(BF16)
    return high, (x - high.astype(F32)).astype(BF16)


def dot(a, b):
    return jnp.dot(a, b, preferred_element_type=F32)


def pieces(lane):
    return (0, lane // 2), (lane // 2, lane // 2)


def flip(index, mask, size):
    bit = 1
    while bit < size:
        if mask & bit:
            index = index + bit - 2 * bit * (index // bit % 2)
        bit *= 2
    return index


def kernel(nx, ny, heads, tok_any, emb_any, qry_any, wk_any, wv_any, wo_any, slot_any, out,
           tok, emb, qry, wk, wo, slot, mixed, wbuf, wsrc, kq_mine, kq_in, kq_all, ex,
           stat, st_in, st2, st2_in, fexp, part, in1, p2, in2, o3, in3, early, spread_ex, tall, fz,
           load_s, send_s, kq_r, z_r, w_r, tok_r, wo_r, st_r, st2_r, s1_r, s2_r, s3_r):
    _, slots, patches, width = tok.shape
    rows = width // ny
    na = ny // CORES
    group = patches // nx
    piece = rows // nx
    lane = width // CORES
    starts, sizes = pieces(lane)
    chunks = len(starts)
    wide = CORES * rows
    first_plane = na // CORES
    own = patches // (nx * ny)
    hdim = width // heads
    lheads = heads // CORES
    cheads = lheads // CORES
    held_slots = CORES * slots
    block_rows = held_slots * group
    scale = 1.0 / math.sqrt(hdim)
    i = lax.axis_index("vx")
    j = lax.axis_index("vy")
    a = j // CORES
    c = j % CORES
    partner = a * CORES + (1 - c)
    x_peers = [flip(i, d, nx) for d in reversed(range(1, nx))]
    mirror = x_peers[0]
    a_peers = [flip(a, d, na) for d in range(1, na)]
    vy_peers = [lax.rem(j + d, ny) for d in range(1, ny)]

    def remote(src, dst, rs, x, y):
        return pltpu.make_async_remote_copy(
            src_ref=src, dst_ref=dst, send_sem=send_s, recv_sem=rs,
            device_id=(x, y), device_id_type=MESH)

    sent = []

    def send(*args):
        copy = remote(*args)
        copy.start()
        sent.append(copy)

    def arrived(ref, rs):
        remote(ref, ref, rs, i, j).wait_recv()

    barrier = pltpu.get_barrier_semaphore()
    for y in vy_peers:
        pl.semaphore_signal(barrier, inc=1, device_id=(i, y), device_id_type=MESH)
    for x in x_peers:
        pl.semaphore_signal(barrier, inc=1, device_id=(x, j), device_id_type=MESH)

    def cols(n):
        return slice(starts[n], starts[n] + sizes[n])

    def quarter(which, n):
        first = (which + CORES * (1 - n)) * sizes[n]
        if isinstance(which, int):
            return wv_any.at[:, first:first + sizes[n]]
        return wv_any.at[:, pl.ds(pl.multiple_of(first, sizes[n]), sizes[n])]

    pairs = ((wk_any, wk), (qry_any, qry),
             (quarter(0, 0), wsrc.at[0, :, cols(0)]), (quarter(1, 0), wsrc.at[1, :, cols(0)]),
             (quarter(0, 1), wsrc.at[0, :, cols(1)]), (quarter(1, 1), wsrc.at[1, :, cols(1)]),
             (quarter(c, 0), wbuf.at[j, :, cols(0)]), (quarter(c, 1), wbuf.at[j, :, cols(1)]),
             (tok_any, tok.at[c]), (emb_any, emb), (slot_any, slot), (wo_any, wo.at[c]))
    loads = [pltpu.make_async_copy(src, dst, load_s.at[n]) for n, (src, dst) in enumerate(pairs)]
    for load in loads:
        load.start()

    with jax.named_scope("A_load01"):
        loads[0].wait()
        loads[1].wait()
    head_row = lax.broadcasted_iota(jnp.int32, (heads, width), 0)
    head_col = lax.broadcasted_iota(jnp.int32, (heads, width), 1) // hdim
    qmat = jnp.where(head_row == head_col, jnp.broadcast_to(qry[...].astype(F32).reshape(1, width), (heads, width)), 0.0).astype(BF16)
    kq = lax.dot_general(qmat, wk[...], NT, preferred_element_type=F32)
    for d in range(CORES):
        for n in range(CORES):
            first = (d + CORES * (1 - n)) * cheads
            kq_high, kq_low = split(kq[first:first + cheads])
            kq_mine[d, 0, n * cheads:(n + 1) * cheads] = kq_high
            kq_mine[d, 1, n * cheads:(n + 1) * cheads] = kq_low

    with jax.named_scope("B_barrier"):
        pl.semaphore_wait(barrier, (ny - 1) + (nx - 1))


    def piece_rows(q):
        return pl.ds(pl.multiple_of(q * piece, piece), piece)

    with jax.named_scope("C_load23"):
        for load in loads[2:6]:
            load.wait()
    def along_z(q, n, x, sem):
        for d in range(CORES):
            send(wsrc.at[d, piece_rows(q), cols(n)], wbuf.at[j, piece_rows(q), cols(n)], sem, i, x * CORES + d)

    for n in range(chunks):
        for x in a_peers:
            along_z(i, n, x, z_r.at[n, a])
            if n == 0 and x is a_peers[-1]:
                for y in vy_peers:
                    send(kq_mine.at[y % CORES], kq_in.at[j], kq_r, i, y)
        if n == 0:
            along_z(mirror, n, a_peers[0], w_r.at[n, a])
        send(wsrc.at[1 - c, :, cols(n)], wbuf.at[j, :, cols(n)], w_r.at[n, a], i, partner)
    with jax.named_scope("C_load4"):
        loads[8].wait()
    send(tok.at[c], tok.at[c], tok_r, i, partner)

    kq_in[j] = kq_mine[c]

    def pair_rows(x, q, n):
        return wbuf.at[pl.ds(pl.multiple_of(x * CORES, CORES), CORES), piece_rows(q), cols(n)]

    def share(n, x):
        here = pair_rows(x, i, n)
        arrived(here, z_r.at[n, x])
        for q in reversed(x_peers[1:] if n > 0 or x is a_peers[0] else x_peers):
            send(here, here, w_r.at[n, x], q, j)

    def complete(n, sources):
        for x in sources:
            if x is a:
                arrived(wbuf.at[partner, :, cols(n)], w_r.at[n, a])
            else:
                arrived(wbuf.at[pl.ds(pl.multiple_of(x * CORES, CORES), CORES), 0:(nx - 1) * piece, cols(n)], w_r.at[n, x])

    with jax.named_scope("D_loads"):
        for load in loads[6:8] + loads[9:]:
            load.wait()
    count = slot.shape[1]
    padded = -(-held_slots // 8) * 8
    ids = (i * ny + a * CORES) * slots + lax.broadcasted_iota(jnp.int32, (padded, count), 0)
    match = jnp.where(ids == jnp.broadcast_to(slot[...], (padded, count)), 1.0, 0.0)
    held = jnp.max(match, axis=1, keepdims=True)
    embed = dot(match.astype(BF16), emb[...])

    def mix(core):
        for s in range(slots):
            m = core * slots + s
            line = jnp.sum(jnp.where(lax.broadcasted_iota(jnp.int32, (padded, width), 0) == m, embed, 0.0), axis=0, keepdims=True)
            for g in range(nx):
                first = pl.multiple_of(g * block_rows + m * group, group)
                mixed[pl.ds(first, group), :] = (tok[core, s, g * group:(g + 1) * group, :].astype(F32) + line).astype(BF16)

    lend = remote(wo.at[0], wo.at[0], wo_r, i, partner)

    @pl.when(c == 0)
    def _():
        lend.start()

    with jax.named_scope("E_mix"):
        mix(c)
    with jax.named_scope("F_share00"):
        share(0, a_peers[0])
    with jax.named_scope("G_tok"):
        arrived(tok.at[1 - c], tok_r)
    with jax.named_scope("G_mix2"):
        mix(1 - c)
    with jax.named_scope("G_share01"):
        for x in a_peers[1:-1]:
            share(0, x)
    for n in range(1, chunks):
        for x in a_peers:
            along_z(mirror, n, x, w_r.at[n, a])
    with jax.named_scope("J_share02"):
        share(0, a_peers[-1])
    with jax.named_scope("H_kq"):
        arrived(kq_in.at[0:ny - 1], kq_r)
    for y in range(ny):
        for d in range(2):
            kq_all[d * lheads:(d + 1) * lheads, y * rows:(y + 1) * rows] = kq_in[y, d]
    for g in range(nx):
        both = lax.dot_general(mixed[g * block_rows:(g + 1) * block_rows, :], kq_all[...], NT, preferred_element_type=F32)
        score = scale * (both[:, 0:lheads] + both[:, lheads:2 * lheads])
        top = jnp.full((group, lheads), LOWEST, F32)
        scores = []
        for s in range(held_slots):
            here = jnp.where(held[s:s + 1, :] > 0, score[s * group:(s + 1) * group], LOWEST)
            scores.append(here)
            top = jnp.maximum(top, here)
        total = jnp.zeros((group, lheads), F32)
        for s in range(held_slots):
            e = jnp.where(held[s:s + 1, :] > 0, jnp.exp(scores[s] - top), 0.0).astype(BF16)
            ex[g * block_rows + s * group:g * block_rows + (s + 1) * group, :] = e
            total += e.astype(F32)
        tall[g * group:(g + 1) * group, 0:lheads] = top
        tall[g * group:(g + 1) * group, lheads:2 * lheads] = total
    flat = tall[...].T
    for g in range(nx):
        stat[g] = flat[0:2 * lheads, g * group:(g + 1) * group]

    def lend_stats():
        return remote(stat.at[i], st_in.at[i * CORES], st_r, i, partner)

    for q in x_peers:
        send(stat.at[q], st_in.at[i * CORES + c], st_r, q, a * CORES + CORES - 1)

    @pl.when(c == 0)
    def _():
        lend_stats().start()

    @pl.when(c == CORES - 1)
    def _():
        st_in[i * CORES + c] = stat[i]

    with jax.named_scope("J_share1"):
        for n in range(1, chunks):
            for x in a_peers:
                share(n, x)

    def group_rows(g):
        return slice(g * block_rows, (g + 1) * block_rows)

    feature = lax.broadcasted_iota(jnp.int32, (lheads, lane), 1)
    spread = jnp.where(feature // hdim == lax.broadcasted_iota(jnp.int32, (lheads, lane), 0), 1.0, 0.0).astype(BF16)

    def plane_product(x, here, where):
        first = pl.multiple_of(x * wide, wide)
        weight = wbuf[pl.ds(pl.multiple_of(x * CORES, CORES), CORES), :, where].reshape(wide, -1)
        return dot(mixed[here, pl.ds(first, wide)], weight)

    def project_early(n, sources, more=False):
        for g in range(nx):
            here = group_rows(g)
            value = sum(plane_product(x, here, cols(n)) for x in sources)
            early[here, cols(n)] = value + early[here, cols(n)] if more else value

    def give(n, g):
        return remote(part.at[n, g], in1.at[n, i * CORES + c], s1_r.at[n], g, a * CORES + CORES - 1)

    def project_late(n, sources):
        for batch in (range(2), range(2, nx)):
            for g in batch:
                here = group_rows(g)
                value = sum(plane_product(x, here, cols(n)) for x in sources)
                value = (value + early[here, cols(n)]) * spread_ex[here, cols(n)]
                part[n, g] = sum(value[s * group:(s + 1) * group] for s in range(held_slots)).astype(BF16)
            for g in batch:
                @pl.when(i != g)
                def _():
                    give(n, g).start()

        for q in x_peers:
            sent.append(give(n, q))

        @pl.when(c == CORES - 1)
        def _():
            in1[n, i * CORES + c] = part[n, i]

        @pl.when(c == 0)
        def _():
            give(n, i).start()

    half_planes = first_plane // CORES
    targets = [(d, k) for d in reversed(range(CORES)) for k in range(half_planes)]

    def target_of(d, k, n):
        return ((d + CORES * (1 - n)) * half_planes + k) * CORES + CORES - 1

    def scatter(d, k, n):
        return remote(p2.at[n, d * half_planes + k], in2.at[a], s2_r, i, target_of(d, k, n))

    def scatter_stats(d, k, n):
        return remote(st2.at[d, n], st2_in.at[a], st2_r, i, target_of(d, k, n))

    def below_of(d):
        tops = [st_in[q * CORES + d, 0:lheads] for q in range(nx)]
        high = functools.reduce(jnp.maximum, tops)
        return high, [jnp.exp(top - high) for top in tops]

    def plane_stats():
        with jax.named_scope("K_st"):
            arrived(st_in.at[0:nx * CORES - 1], st_r)
        for d in range(CORES):
            high, below = below_of(d)
            total = sum(below[q] * st_in[q * CORES + d, lheads:2 * lheads] for q in range(nx))
            for n in range(chunks):
                heads_n = slice(n * cheads, (n + 1) * cheads)
                st2[d, n, 0:cheads] = high[heads_n]
                st2[d, n, cheads:lheads] = total[heads_n]
        for n in range(chunks):
            for d, k in targets:
                @pl.when(target_of(d, k, n) != j)
                def _():
                    scatter_stats(d, k, n).start()

    def plane_factors():
        for d in range(CORES):
            _, below = below_of(d)
            for q in range(nx):
                f_high, f_low = split(below[q])
                fexp[q * CORES + d] = (lax.dot_general(f_high, spread, TN, preferred_element_type=F32)
                                       + lax.dot_general(f_low, spread, TN, preferred_element_type=F32))

    def combine(n):
        arrived(in1.at[n, 0:nx * CORES - 1], s1_r.at[n])
        for d in reversed(range(CORES)):
            acc = sum(fexp[q * CORES + d, :, cols(n)] * in1[n, q * CORES + d].astype(F32) for q in range(nx))
            for k in range(half_planes):
                p2[n, d * half_planes + k] = acc[:, k * wide:(k + 1) * wide].astype(BF16)

                @pl.when(target_of(d, k, n) != j)
                def _():
                    scatter(d, k, n).start()

    spread_ex[...] = dot(ex[...], spread)
    with jax.named_scope("K_complete0"):
        complete(0, [a] + a_peers[:-2])
    with jax.named_scope("K_early0"):
        project_early(0, [a] + a_peers[:-2])
    with jax.named_scope("L_complete0"):
        complete(0, a_peers[-2:])
    with jax.named_scope("M_project0"):
        project_late(0, a_peers[-2:])
    @pl.when(c == CORES - 1)
    def _():
        plane_stats()

    for n in range(1, chunks):
        with jax.named_scope("O_early1"):
            complete(n, [a])
            project_early(n, [a])
        with jax.named_scope("O_complete1"):
            complete(n, a_peers[:-1])
        with jax.named_scope("O_early2"):
            project_early(n, a_peers[:-1], True)
        with jax.named_scope("O_complete2"):
            complete(n, a_peers[-1:])
        with jax.named_scope("P_project1"):
            project_late(n, a_peers[-1:])
    block = a // half_planes
    spot = lax.rem(a, half_planes)
    my_chunk = 1 - block // CORES
    my_lane = lax.rem(block, CORES)
    root_first = [k + (k + na - a) // na for k in range(na - 1)]

    @pl.when(c == CORES - 1)
    def _():
        plane_factors()
        for n in range(chunks):
            with jax.named_scope(f"R_combine{n}"):
                combine(n)
        st2_in[a] = st2[my_lane, my_chunk]
        in2[a] = p2[my_chunk, my_lane * half_planes + spot]
        arrived(st2_in.at[0:na - 1], st2_r)

        highest = functools.reduce(jnp.maximum, [st2_in[p, 0:cheads] for p in range(na)])
        lower = [jnp.exp(st2_in[p, 0:cheads] - highest) for p in range(na)]
        whole = sum(lower[p] * st2_in[p, cheads:lheads] for p in range(na))
        wanted = (spot * wide + lax.broadcasted_iota(jnp.int32, (cheads, wide), 1)) // hdim
        widen = jnp.where(wanted == lax.broadcasted_iota(jnp.int32, (cheads, wide), 0), 1.0, 0.0).astype(BF16)
        for p in range(na):
            f_high, f_low = split(lower[p] / whole)
            fz[p] = (lax.dot_general(f_high, widen, TN, preferred_element_type=F32)
                     + lax.dot_general(f_low, widen, TN, preferred_element_type=F32))
        arrived(wo.at[0], wo_r)

        with jax.named_scope("S_in2"):
            arrived(in2.at[0:na - 1], s2_r)

        acc = sum(fz[p] * in2[p].astype(F32) for p in range(na))
        result = dot(acc.astype(BF16), wo[...].reshape(wide, width)).astype(BF16)
        for y in range(ny):
            o3[y] = result[y * own:(y + 1) * own]
        for x in root_first:
            for d in range(CORES):
                remote(o3.at[x * CORES + d], in3.at[a], s3_r, i, x * CORES + d).start()
        remote(o3.at[partner], in3.at[a], s3_r, i, partner).start()
        in3[a] = o3[j]
        with jax.named_scope("T_in3n"):
            arrived(in3.at[0:na - 1], s3_r)

    @pl.when(c != CORES - 1)
    def _():
        with jax.named_scope("T_in3s"):
            arrived(in3, s3_r)

    final = sum(in3[x].astype(F32) for x in range(na))
    out[...] = final.astype(BF16)
    with jax.named_scope("U_sends"):
        for copy in sent:
            copy.wait_send()
    @pl.when(c == 0)
    def _():
        lend.wait_send()
        lend_stats().wait_send()
        for n in range(chunks):
            give(n, i).wait_send()

    @pl.when(c == CORES - 1)
    def _():
        for n in range(chunks):
            for d, k in targets:
                @pl.when(target_of(d, k, n) != j)
                def _():
                    scatter(d, k, n).wait_send()
                    scatter_stats(d, k, n).wait_send()
        for y in vy_peers:
            remote(o3.at[y], in3.at[a], s3_r, i, y).wait_send()


def shards(tokens, var_embed, query, key_weight, value_weight, out_weight, var_slot):
    slots, batch, patches, width = tokens.shape
    nx, ny = lax.axis_size("vx"), lax.axis_size("vy")
    heads = HEADS
    patches = batch * patches
    rows, na, group, own = width // ny, ny // CORES, patches // nx, patches // (nx * ny)
    lane, lheads = width // CORES, heads // CORES
    chunks = len(pieces(lane)[0])
    held = CORES * slots * patches
    dma = pltpu.SemaphoreType.DMA
    vmem = pltpu.VMEM
    result = pl.pallas_call(
        functools.partial(kernel, nx, ny, heads),
        out_shape=vmem((own, width), BF16),
        in_specs=[pl.BlockSpec(memory_space=pl.ANY)] * 7,
        out_specs=pl.BlockSpec(memory_space=vmem),
        scratch_shapes=[
            vmem((CORES, slots, patches, width), BF16),
            vmem(var_embed.shape, BF16),
            vmem((width,), BF16),
            vmem((rows, width), BF16),
            vmem((CORES, rows, width), BF16),
            vmem((1, var_slot.shape[0]), jnp.int32),
            vmem((held, width), BF16),
            vmem((ny, rows, lane), BF16),
            vmem((CORES, rows, lane), BF16),
            vmem((CORES, 2, lheads, rows), BF16),
            vmem((ny, 2, lheads, rows), BF16),
            vmem((2 * lheads, width), BF16),
            vmem((held, lheads), BF16),
            vmem((nx, 2 * lheads, group), F32),
            vmem((nx * CORES, 2 * lheads, group), F32),
            vmem((CORES, chunks, lheads, group), F32),
            vmem((na, lheads, group), F32),
            vmem((nx * CORES, group, lane), F32),
            vmem((chunks, nx, group, lane // chunks), BF16),
            vmem((chunks, nx * CORES, group, lane // chunks), BF16),
            vmem((chunks, na // CORES, group, CORES * rows), BF16),
            vmem((na, group, CORES * rows), BF16),
            vmem((ny, own, width), BF16),
            vmem((na, own, width), BF16),
            vmem((held, lane), F32),
            vmem((held, lane), F32),
            vmem((patches, 128), F32),
            vmem((na, group, CORES * rows), F32),
            dma((12,)), dma, dma, dma((chunks, na)), dma((chunks, na)), dma, dma, dma, dma,
            dma((chunks,)), dma, dma,
        ],
        compiler_params=pltpu.CompilerParams(
            collective_id=0, has_side_effects=True, vmem_limit_bytes=56 * 1024 * 1024),
    )(
        tokens.reshape(slots, patches, width), var_embed, query,
        key_weight, value_weight, out_weight, var_slot.reshape(1, -1),
    )
    return result.reshape(batch, -1, width)


def solution(mesh):
    placed = (
        P(("vx", "vy"), None, None, None),
        P(),
        P(),
        P("vy", None),
        P("vy", None),
        P("vy", None),
        P(),
    )
    return jax.shard_map(
        shards, mesh=mesh, in_specs=placed, out_specs=P(None, ("vx", "vy"), None), check_vma=False
    )
```
